32 devices in a mesh: dp: 4 (over y, x), tensor: 8 (over z, core).
Axes of the slice: x: 2, y: 2, z: 4, core: 2. Of those that a mesh axis runs over, the one named last changes fastest.
Arguments:
- tokens: bfloat16 [2048, 4096], P(('dp', 'tensor')), parts along dimension 0, may hold values from -6 to 6
- norm_gain: float32 [4096], replicated, may hold values from 0.5 to 1.5
- gate_weight: bfloat16 [4096, 14336], P(None, 'tensor'), may hold values from -0.09375 to 0.09375
- up_weight: bfloat16 [4096, 14336], P(None, 'tensor'), may hold values from -0.09375 to 0.09375
- down_weight: bfloat16 [14336, 4096], P('tensor'), may hold values from -0.0625 to 0.0625
Outputs:
- mixed: bfloat16 [2048, 4096], P('dp', 'tensor'), parts along dimension 0
The draws below stay inside these ranges and needn't reach their ends.
There are 4 independent parts, one for each index of `dp`. The reference program is written for one: setup_inputs(seed, part) draws one part's arguments, and reference() takes and returns one part's arrays. A program takes and returns all parts, laid end to end along the dimension named above; an argument that names none is the same for every part. Nothing has to cross between parts.
All inputs are finite; a program needn't handle non-finite values.
Results may differ from the reference program's by a relative error of at most 0.0053.
Values may be sent and summed in bfloat16 or wider, within the bound.
A program may use at most 128 MiB of HBM per device.

```python
import jax
import jax.numpy as jnp
from jax import lax

D = 4096
FF = 14336
TOKENS = 512


def raised(entries, key, source, target, blocks, factor):
    owner, partner = [(jnp.arange(entries.shape[axis_at]) // (entries.shape[axis_at] // blocks)).reshape([-1 if axis == axis_at else 1 for axis in range(entries.ndim)]) for axis_at in (source, target)]
    chosen = jax.random.permutation(key, blocks)[partner]
    strong = (owner == chosen) | (owner == (partner + blocks // 2) % blocks)
    return jnp.where(strong, factor * entries, entries)


def levels(rng, extent, cuts, smallest, high):
    factor_of = 1.0
    for axis_at, parts in cuts:
        heights = jax.random.uniform(jax.random.fold_in(jax.random.fold_in(rng, 6), axis_at), (parts,), jnp.float32, smallest / len(cuts), high / len(cuts))
        factor_of = factor_of * jnp.repeat(jnp.exp(heights), extent[axis_at] // parts).reshape((-1,) + (1,) * (len(extent) - 1 - axis_at))
    return factor_of


def centred(stream_key, dims, spread, most, cuts=(), dtype=jnp.bfloat16):
    gain = levels(stream_key, dims, cuts, -0.22, 0.18) if cuts else 1.0
    drawn = jax.random.normal(stream_key, dims, jnp.float32) * spread * gain
    return jnp.minimum(jnp.maximum(drawn, -most), most).astype(dtype)


def bell_draw_with(rng, extent, spread, bound, shards, heavy, held_as=jnp.bfloat16):
    entries = spread * jax.random.normal(rng, extent, jnp.float32)
    if shards:
        entries = entries * levels(rng, extent, shards, -0.22, 0.18)
    return jnp.clip(raised(entries, jax.random.fold_in(rng, 3), *heavy), -bound, bound).astype(held_as)


def setup_inputs(seed: int = 0, part: int = 0) -> dict:
    streams_of = jax.random.split(jax.random.key(seed), 6)
    part_keys = jax.random.split(jax.random.fold_in(streams_of[5], part), 6)
    tokens = centred(part_keys[0], (TOKENS, D), 1.0, 6.0, ((0, 8),))
    norm_gain = jnp.clip(1.0 + 0.1 * jax.random.normal(streams_of[1], (D,), jnp.float32), 0.5, 1.5)
    gate_weight = centred(streams_of[2], (D, FF), D ** -0.5, 0.09375, ((1, 8),))
    up_weight = centred(streams_of[3], (D, FF), D ** -0.5, 0.09375, ((1, 8),))
    down_weight = bell_draw_with(streams_of[4], (FF, D), FF ** -0.5, 0.0625, ((0, 8),), (0, 1, 8, 2.0))
    return {"tokens": tokens, "norm_gain": norm_gain, "gate_weight": gate_weight, "up_weight": up_weight, "down_weight": down_weight}


def reference(tokens, norm_gain, gate_weight, up_weight, down_weight):
    wide = tokens.astype(jnp.float32)
    square_mean = lax.optimization_barrier(jnp.mean(wide * wide, axis=1, keepdims=True))
    normed = (wide * norm_gain[None, :] / jnp.sqrt(square_mean + 1e-05)).astype(jnp.bfloat16)
    gate = jnp.dot(normed, gate_weight, preferred_element_type=jnp.float32)
    up = jnp.dot(normed, up_weight, preferred_element_type=jnp.float32)
    hidden = (jax.nn.silu(gate) * up).astype(jnp.bfloat16)
    branch = jnp.dot(hidden, down_weight, preferred_element_type=jnp.float32)
    return (wide + branch).astype(jnp.bfloat16)
```

```python
import functools

import jax
import jax.numpy as jnp
from jax import lax
from jax.experimental import pallas as pl
from jax.experimental.pallas import tpu as pltpu
from jax.sharding import PartitionSpec as P

SUBS = 2
VMEM_LIMIT = 67043328
f32, bf16 = jnp.float32, jnp.bfloat16


def tile_of(F):
    return next(t for t in (896, 512, 256, 128) if F % t == 0)


def block_kernel(
    n, tok, gain, gw, uw, dw, out,
    gwv, uwv, dwv, every, normed, hidden, mine, theirs, peer, arrived, far, acc,
    load_sem, own_sem, ag_recv, ag_send, peer_send, peer_recv, rs_send, rs_recv, far_recv,
):
    S = SUBS
    dp = lax.axis_index("dp")
    me = lax.axis_index("tensor")
    C = n // 2
    p, c = me // 2, me % 2
    R, D = tok.shape
    Rs = R // S
    T = 2 * R
    F = gwv.shape[1]
    W = D // n
    tile = tile_of(F)
    tiles = F // tile
    partner = (dp, 2 * p + (1 - c))
    right = (dp, lax.rem(me + 2, n))
    left = (dp, lax.rem(me + n - 2, n))
    first, last = (dp, c), (dp, 2 * (C - 1) + c)
    has_right, has_left = p < C - 1, p > 0
    leans_left = 2 * p < C - 1
    near = jnp.where(leans_left, -1, 1)
    both = jnp.where(leans_left, p, C - 1 - p)

    def rows_of(b, j, q):
        return pl.ds(pl.multiple_of(((b * S + j) * 2 + q) * Rs, Rs), Rs)

    def block_rows(b):
        return pl.ds(pl.multiple_of(b * T, T), T)

    def columns(t):
        return pl.ds(pl.multiple_of(t * W, W), W)

    own = [pltpu.make_async_copy(tok.at[pl.ds(j * Rs, Rs), :], every.at[rows_of(p, j, c), :], own_sem.at[j]) for j in range(S)]

    def load_tile(i):
        at = pl.ds(i * tile, tile)
        return (
            pltpu.make_async_copy(gw.at[:, at], gwv.at[:, at], load_sem.at[2 * i]),
            pltpu.make_async_copy(uw.at[:, at], uwv.at[:, at], load_sem.at[2 * i + 1]),
        )

    load_down = pltpu.make_async_copy(dw, dwv, load_sem.at[2 * tiles])

    for copy in own:
        copy.start()
    for i in range(tiles):
        for copy in load_tile(i):
            copy.start()

    barrier = pltpu.get_barrier_semaphore()

    def greet(device):
        pl.semaphore_signal(barrier, inc=1, device_id=device, device_id_type=pl.DeviceIdType.MESH)

    greet(partner)
    pl.when(has_right)(lambda: greet(right))
    pl.when(has_left)(lambda: greet(left))
    pl.when(p >= 2)(lambda: greet(first))
    pl.when(p <= C - 3)(lambda: greet(last))
    ends = (p == 0).astype(jnp.int32) + (p == C - 1).astype(jnp.int32)
    pl.semaphore_wait(barrier, 1 + has_right.astype(jnp.int32) + has_left.astype(jnp.int32) + ends * (C - 2))

    def remote(src, dst, s, d, device):
        return pltpu.make_async_remote_copy(
            src_ref=src, dst_ref=dst, send_sem=s, recv_sem=d, device_id=device, device_id_type=pl.DeviceIdType.MESH
        )

    def gather(b, j, way):
        at = every.at[rows_of(b, j, c), :]
        return remote(at, at, ag_send.at[way, b, j], ag_recv.at[b, j, c], (right, left, partner)[way])

    def gathered(b, j, q):
        at = every.at[rows_of(b, j, q), :]
        remote(at, at, ag_send.at[2, b, j], ag_recv.at[b, j, q], partner).wait_recv()

    def relay(k, j):
        @pl.when(p - k >= 0)
        def _():
            gathered(p - k, j, c)
            pl.when(has_right)(lambda: gather(p - k, j, 0).start())
            gather(p - k, j, 2).start()

        @pl.when(p + k <= C - 1)
        def _():
            gathered(p + k, j, c)
            pl.when(has_left)(lambda: gather(p + k, j, 1).start())
            gather(p + k, j, 2).start()

    def to_peer(b, d):
        return remote(theirs.at[b, d], peer.at[b, d], peer_send.at[b, d], peer_recv.at[b, d], partner)

    def to_right(b, d):
        return remote(mine.at[b, d], arrived.at[b, d + 1], rs_send.at[b, d], rs_recv.at[b, d + 1], right)

    def to_left(b, d):
        return remote(mine.at[b, d], arrived.at[b, d], rs_send.at[b, d], rs_recv.at[b, d], left)

    def to_far(side, b, d):
        return remote(mine.at[b, d], far.at[side], rs_send.at[b, d], far_recv.at[side], (dp, 2 * d + c))

    def landed(b, slot):
        remote(arrived.at[b, slot], arrived.at[b, slot], rs_send.at[b, 0], rs_recv.at[b, slot], partner).wait_recv()

    def landed_far(side):
        remote(far.at[side], far.at[side], rs_send.at[0, 0], far_recv.at[side], partner).wait_recv()

    def first_send(b, d):
        rightward, leftward = d > p, d < p
        straight = (p == 0) & (b == C - 1) & (d >= 2)
        pl.when(straight)(lambda: to_far(0, b, d).start())
        pl.when(rightward & ((p == 0) | ((p == 1) & (b == C - 1))) & jnp.logical_not(straight))(lambda: to_right(b, d).start())
        straight_left = (p == C - 1) & (b == 0) & (d <= C - 3)
        pl.when(straight_left)(lambda: to_far(1, b, d).start())
        pl.when(leftward & ((p == C - 1) | ((p == C - 2) & (b == 0))) & jnp.logical_not(straight_left))(lambda: to_left(b, d).start())

    def add_to_mine(b, d, slot):
        landed(b, slot)
        mine[b, d] = (mine[b, d].astype(f32) + arrived[b, slot].astype(f32)).astype(bf16)

    def forward_right(b):
        for i in range(C - 1):
            d = C - 1 - i

            @pl.when(d > p)
            def _():
                add_to_mine(b, d, d + 1)
                to_right(b, d).start()

    def forward_left(b):
        for d in range(C - 1):
            @pl.when(d < p)
            def _():
                add_to_mine(b, d, d)
                to_left(b, d).start()

    def early(b):
        pl.when((p == 1) & has_right)(lambda: forward_right(b))
        pl.when((p == C - 2) & has_left)(lambda: forward_left(C - 1 - b))

    def final(b):
        acc_b = acc.at[block_rows(b), :]

        @pl.when(has_left)
        def _():
            landed(b, p + 1)
            acc_b[...] += arrived[b, p + 1].astype(f32)

        @pl.when(has_right)
        def _():
            landed(b, p)
            acc_b[...] += arrived[b, p].astype(f32)

        @pl.when((b == C - 1) & (p >= 2))
        def _():
            landed_far(0)
            acc_b[...] += far[0].astype(f32)

        @pl.when((b == 0) & (p <= C - 3))
        def _():
            landed_far(1)
            acc_b[...] += far[1].astype(f32)

        for j in range(S):
            for q in range(2):
                at = pl.ds(pl.multiple_of((2 * b + q) * R + j * Rs, Rs), Rs)
                out[at, :] = acc[rows_of(b, j, q), :].astype(bf16)

    def norm(b):
        step = 32

        @pl.loop(0, T // step)
        def _(i):
            at = pl.ds(pl.multiple_of(b * T + i * step, step), step)
            wide = every[at, :].astype(f32)
            scale = 1.0 / jnp.sqrt(jnp.mean(wide * wide, axis=1, keepdims=True) + 1e-05)
            normed[pl.ds(pl.multiple_of(i * step, step), step), :] = (wide * gain[...] * scale).astype(bf16)

    def expand(s):
        @pl.loop(0, tiles)
        def _(i):
            @pl.when((s == 0) & (i == tiles - 1))
            def _():
                relay(1, 0)

            @pl.when(s == 0)
            def _():
                for x in range(tiles):
                    @pl.when(i == x)
                    def _():
                        for copy in load_tile(x):
                            copy.wait()

                pl.when(i == 0)(lambda: load_down.start())

            at = pl.ds(pl.multiple_of(i * tile, tile), tile)
            gate = jnp.dot(normed[...], gwv[:, at], preferred_element_type=f32)
            up = jnp.dot(normed[...], uwv[:, at], preferred_element_type=f32)
            hidden[:, at] = (jax.nn.silu(gate) * up).astype(bf16)

    def down(b):
        def dest(i):
            return jnp.where(leans_left, C - 1 - i, i)

        @pl.loop(0, C)
        def _(i):
            d = dest(i)
            theirs[b, d] = jnp.dot(hidden[...], dwv[:, columns(2 * d + 1 - c)], preferred_element_type=f32).astype(bf16)
            to_peer(b, d).start()

        @pl.loop(0, C)
        def _(i):
            d = dest(i)
            to_peer(b, d).wait_recv()
            total = jnp.dot(hidden[...], dwv[:, columns(2 * d + c)], preferred_element_type=f32) + peer[b, d].astype(f32)
            mine[b, d] = total.astype(bf16)

            @pl.when(d == p)
            def _():
                acc[block_rows(b), :] = every[block_rows(b), columns(me)].astype(f32) + mine[b, d].astype(f32)

            first_send(b, d)

    for j in range(S):
        own[j].wait()
        pl.when(has_right)(lambda: gather(p, j, 0).start())
        pl.when(has_left)(lambda: gather(p, j, 1).start())
        gather(p, j, 2).start()

    @pl.loop(0, C)
    def _(s):
        k = jnp.where(s <= 2 * both, (s + 1) // 2, s - both)
        side = jnp.where((s <= 2 * both) & (s % 2 == 1), near, -near)
        b = p + side * k

        pl.when((s >= 1) & (k == s))(lambda: relay(s, 1))
        for j in range(S):
            gathered(b, j, 1 - c)
        norm(b)
        expand(s)
        pl.when((s >= 1) & (k != s))(lambda: relay(s, 1))
        pl.when((s >= 1) & (s + 1 <= C - 1))(lambda: relay(s + 1, 0))
        pl.when(s >= 3)(lambda: early(s - 2))
        pl.when(s == 0)(lambda: load_down.wait())
        down(b)
        pl.when(s == 1)(lambda: early(0))

    order = [*range(C - 2), C - 1, C - 2]
    for b in order:
        passes = has_left & has_right & jnp.logical_not((p == 1) & ((b == C - 1) | (b <= C - 3)))
        pl.when(passes)(lambda: forward_right(b))
        passes = has_left & has_right & jnp.logical_not((p == C - 2) & ((b == C - 1) | (b <= C - 3)))
        pl.when(passes)(lambda: forward_left(C - 1 - b))
    for b in order:
        final(jnp.where(leans_left, C - 1 - b, b))

    for b in range(C):
        for j in range(S):
            pl.when((b <= p) & has_right)(lambda: gather(b, j, 0).wait_send())
            pl.when((b >= p) & has_left)(lambda: gather(b, j, 1).wait_send())
            gather(b, j, 2).wait_send()
        for d in range(C):
            to_peer(b, d).wait_send()
            pl.when(d != p)(lambda: to_right(b, d).wait_send())


def on_device(n, tokens, norm_gain, gate_weight, up_weight, down_weight):
    S = SUBS
    R, D = tokens.shape
    F = gate_weight.shape[1]
    C = n // 2
    T, W = 2 * R, D // n
    any_space, vmem = pl.BlockSpec(memory_space=pl.ANY), pl.BlockSpec(memory_space=pltpu.VMEM)
    dma = pltpu.SemaphoreType.DMA
    return pl.pallas_call(
        functools.partial(block_kernel, n),
        out_shape=jax.ShapeDtypeStruct((n * R, W), bf16),
        in_specs=[any_space, vmem, any_space, any_space, any_space],
        out_specs=vmem,
        scratch_shapes=[
            pltpu.VMEM((D, F), bf16),
            pltpu.VMEM((D, F), bf16),
            pltpu.VMEM((F, D), bf16),
            pltpu.VMEM((C * T, D), bf16),
            pltpu.VMEM((T, D), bf16),
            pltpu.VMEM((T, F), bf16),
            pltpu.VMEM((C, C, T, W), bf16),
            pltpu.VMEM((C, C, T, W), bf16),
            pltpu.VMEM((C, C, T, W), bf16),
            pltpu.VMEM((C, C + 1, T, W), bf16),
            pltpu.VMEM((2, T, W), bf16),
            pltpu.VMEM((C * T, W), f32),
            dma((2 * (F // tile_of(F)) + 1,)),
            dma((S,)),
            dma((C, S, 2)),
            dma((3, C, S)),
            dma((C, C)),
            dma((C, C)),
            dma((C, C)),
            dma((C, C + 1)),
            dma((2,)),
        ],
        compiler_params=pltpu.CompilerParams(collective_id=0, has_side_effects=True, vmem_limit_bytes=VMEM_LIMIT),
    )(tokens, norm_gain[None, :], gate_weight, up_weight, down_weight)


def solution(mesh):
    return jax.shard_map(
        functools.partial(on_device, mesh.shape["tensor"]),
        mesh=mesh,
        in_specs=(
            P(("dp", "tensor"), None),
            P(),
            P(None, "tensor"),
            P(None, "tensor"),
            P("tensor", None),
        ),
        out_specs=P("dp", "tensor"),
        check_vma=False,
    )
```

```python
import functools

import jax
import jax.numpy as jnp
from jax import lax
from jax.experimental import pallas as pl
from jax.experimental.pallas import tpu as pltpu
from jax.sharding import PartitionSpec as P

SUBS = 2
VMEM_LIMIT = 67043328
f32, bf16 = jnp.float32, jnp.bfloat16


def tile_of(F):
    return next(t for t in (256, 128) if F % t == 0)


def block_kernel(
    n, tok, gain, gw, uw, dw, out,
    gwv, uwv, dwv, every, normed, hidden, half, outv, mine, theirs, peer, arrived, far, acc,
    load_sem, own_sem, ag_recv, ag_send, peer_send, peer_recv, rs_send, rs_recv, far_recv, out_sem,
):
    S = SUBS
    dp = lax.axis_index("dp")
    me = lax.axis_index("tensor")
    C = n // 2
    p, c = me // 2, me % 2
    R, D = tok.shape
    Rs = R // S
    T = 2 * R
    F = gwv.shape[1]
    W = D // n
    tile = tile_of(F)
    tiles = F // tile
    cuts = [0, (tiles + 1) // 2, tiles]
    partner = (dp, 2 * p + (1 - c))
    right = (dp, lax.rem(me + 2, n))
    left = (dp, lax.rem(me + n - 2, n))
    has_right, has_left = p < C - 1, p > 0
    inner = has_right & has_left
    outer = jnp.logical_not(inner)
    leans_left = 2 * p < C - 1
    near = jnp.where(leans_left, -1, 1)
    both = jnp.where(leans_left, p, C - 1 - p)

    def rows_of(b, j, q):
        return pl.ds(pl.multiple_of(((b * S + j) * 2 + q) * Rs, Rs), Rs)

    def block_rows(b):
        return pl.ds(pl.multiple_of(b * T, T), T)

    def columns(t):
        return pl.ds(pl.multiple_of(t * W, W), W)

    own = [pltpu.make_async_copy(tok.at[pl.ds(j * Rs, Rs), :], every.at[rows_of(p, j, c), :], own_sem.at[j]) for j in range(S)]

    def load_wide(i):
        at = pl.ds(cuts[i] * tile, (cuts[i + 1] - cuts[i]) * tile)
        return (
            pltpu.make_async_copy(gw.at[:, at], gwv.at[:, at], load_sem.at[2 * i]),
            pltpu.make_async_copy(uw.at[:, at], uwv.at[:, at], load_sem.at[2 * i + 1]),
        )

    def load_down(q, d):
        return pltpu.make_async_copy(
            dw.at[:, columns(2 * d + q)], dwv.at[q, :, pl.ds(d * W, W)], load_sem.at[4 + C * q + d]
        )

    for copy in own:
        copy.start()

    barrier = pltpu.get_barrier_semaphore()

    def greet(device):
        pl.semaphore_signal(barrier, inc=1, device_id=device, device_id_type=pl.DeviceIdType.MESH)

    greet(partner)
    pl.when(has_right)(lambda: greet(right))
    pl.when(has_left)(lambda: greet(left))
    with jax.named_scope("own"):
        for copy in own:
            copy.wait()
    for i in range(2):
        for copy in load_wide(i):
            copy.start()
    with jax.named_scope("barrier"):
        pl.semaphore_wait(barrier, 1 + has_right.astype(jnp.int32) + has_left.astype(jnp.int32))

    def remote(src, dst, s, d, device):
        return pltpu.make_async_remote_copy(
            src_ref=src, dst_ref=dst, send_sem=s, recv_sem=d, device_id=device, device_id_type=pl.DeviceIdType.MESH
        )

    def gather(b, j, way):
        at = every.at[rows_of(b, j, c), :]
        return remote(at, at, ag_send.at[way, b, j], ag_recv.at[b, j, c], (right, left, partner)[way])

    def gathered(b, j, q):
        at = every.at[rows_of(b, j, q), :]
        remote(at, at, ag_send.at[2, b, j], ag_recv.at[b, j, q], partner).wait_recv()

    @jax.named_scope("relay")
    def relay(k, j):
        @pl.when(p - k >= 0)
        def _():
            gathered(p - k, j, c)
            pl.when(has_right)(lambda: gather(p - k, j, 0).start())
            gather(p - k, j, 2).start()

        @pl.when(p + k <= C - 1)
        def _():
            gathered(p + k, j, c)
            pl.when(has_left)(lambda: gather(p + k, j, 1).start())
            gather(p + k, j, 2).start()

    def to_peer(b, d):
        return remote(theirs.at[b, d], peer.at[b, d], peer_send.at[b, d], peer_recv.at[b, d], partner)

    def to_right(b, d):
        return remote(mine.at[b, d], arrived.at[b, d + 1], rs_send.at[b, d], rs_recv.at[b, d + 1], right)

    def to_left(b, d):
        return remote(mine.at[b, d], arrived.at[b, d], rs_send.at[b, d], rs_recv.at[b, d], left)

    def to_far(side, b, d):
        return remote(mine.at[b, d], far.at[side], rs_send.at[b, d], far_recv.at[side], (dp, 2 * d + c))

    def landed(b, slot):
        remote(arrived.at[b, slot], arrived.at[b, slot], rs_send.at[b, 0], rs_recv.at[b, slot], partner).wait_recv()

    def landed_far(side):
        remote(far.at[side], far.at[side], rs_send.at[0, 0], far_recv.at[side], partner).wait_recv()

    def straight_right(b, d):
        return (C > 2) & (b == C - 1) & (d == C - 1)

    def straight_left(b, d):
        return (C > 2) & (b == 0) & (d == 0)

    def first_send(b, d):
        straight = straight_right(b, d)
        pl.when((p == 0) & straight)(lambda: to_far(0, b, d).start())
        pl.when((d > p) & jnp.where(straight, p == 1, p == 0))(lambda: to_right(b, d).start())
        straight = straight_left(b, d)
        pl.when((p == C - 1) & straight)(lambda: to_far(1, b, d).start())
        pl.when((d < p) & jnp.where(straight, p == C - 2, p == C - 1))(lambda: to_left(b, d).start())

    def add_to_mine(b, d, slot):
        landed(b, slot)
        mine[b, d] = (mine[b, d].astype(f32) + arrived[b, slot].astype(f32)).astype(bf16)

    @jax.named_scope("right")
    def forward_right(b):
        for i in range(C - 1):
            d = C - 1 - i

            @pl.when((d > p) & jnp.logical_not((p == 1) & straight_right(b, d)))
            def _():
                add_to_mine(b, d, d + 1)
                to_right(b, d).start()

    @jax.named_scope("left")
    def forward_left(b):
        for d in range(C - 1):
            @pl.when((d < p) & jnp.logical_not((p == C - 2) & straight_left(b, d)))
            def _():
                add_to_mine(b, d, d)
                to_left(b, d).start()

    def early(b):
        pl.when((p == 1) & has_right)(lambda: forward_right(b))
        pl.when((p == C - 2) & has_left)(lambda: forward_left(C - 1 - b))

    def earlier():
        pl.when((p == 2) & has_right)(lambda: forward_right(1))
        pl.when((p == C - 3) & has_left)(lambda: forward_left(C - 2))

    @jax.named_scope("final")
    def final(b):
        acc_b = acc.at[block_rows(b), :]

        @pl.when(has_left)
        def _():
            landed(b, p + 1)
            acc_b[...] += arrived[b, p + 1].astype(f32)

        @pl.when(has_right)
        def _():
            landed(b, p)
            acc_b[...] += arrived[b, p].astype(f32)

        @pl.when(straight_right(b, p))
        def _():
            landed_far(0)
            acc_b[...] += far[0].astype(f32)

        @pl.when(straight_left(b, p))
        def _():
            landed_far(1)
            acc_b[...] += far[1].astype(f32)

        for j in range(S):
            for q in range(2):
                outv[b, pl.ds(q * R + j * Rs, Rs), :] = acc[rows_of(b, j, q), :].astype(bf16)

        store(b).start()

    def store(b):
        return pltpu.make_async_copy(outv.at[b], out.at[block_rows(b), :], out_sem.at[b])

    @jax.named_scope("norm")
    def norm(b):
        step = 32

        @pl.loop(0, T // step)
        def _(i):
            at = pl.ds(pl.multiple_of(b * T + i * step, step), step)
            wide = every[at, :].astype(f32)
            scale = 1.0 / jnp.sqrt(jnp.mean(wide * wide, axis=1, keepdims=True) + 1e-05)
            normed[pl.ds(pl.multiple_of(i * step, step), step), :] = (wide * gain[...] * scale).astype(bf16)

    def expand(s):
        def part(i):
            for x in range(cuts[i], cuts[i + 1]):
                at = pl.ds(x * tile, tile)
                gate = jnp.dot(normed[...], gwv[:, at], preferred_element_type=f32)
                up = jnp.dot(normed[...], uwv[:, at], preferred_element_type=f32)
                hidden[:, at] = (jax.nn.silu(gate) * up).astype(bf16)

        @pl.when(s == 0)
        def _():
            with jax.named_scope("load"):
                for copy in load_wide(0):
                    copy.wait()
                for q in range(2):
                    for d in range(C):
                        load_down(jnp.where(c == 0, 1 - q, q), d).start()

        with jax.named_scope("expand0"):
            part(0)
        pl.when(inner & (s <= 1))(lambda: relay(s + 1, 0))

        @pl.when(s == 0)
        def _():
            with jax.named_scope("load"):
                for copy in load_wide(1):
                    copy.wait()

        with jax.named_scope("expand1"):
            part(1)

    def down(b, s):
        def dest(i):
            return jnp.where(leans_left, C - 1 - i, i)

        def product(q, d):
            return jnp.dot(hidden[...], dwv[q, :, pl.ds(d * W, W)], preferred_element_type=f32)

        @pl.when(s == 0)
        def _():
            with jax.named_scope("load"):
                for d in range(C):
                    load_down(1 - c, d).wait()

        with jax.named_scope("down0"):
            for d in range(C):
                theirs[b, d] = product(1 - c, d).astype(bf16)
        for i in range(C):
            to_peer(b, dest(i)).start()

        pl.when(inner & (s <= 1))(lambda: relay(s + 1, 1))
        pl.when(s >= 2)(lambda: early(s - 1))

        @pl.when(s == 0)
        def _():
            with jax.named_scope("load"):
                for d in range(C):
                    load_down(c, d).wait()

        with jax.named_scope("down1"):
            for d in range(C):
                half[d] = product(c, d)
        for i in range(C):
            d = dest(i)
            with jax.named_scope("peer"):
                to_peer(b, d).wait_recv()
            mine[b, d] = (half[d] + peer[b, d].astype(f32)).astype(bf16)
            first_send(b, d)

        acc[block_rows(b), :] = every[block_rows(b), columns(me)].astype(f32) + mine[b, p].astype(f32)

    for j in range(S):
        pl.when(has_right)(lambda: gather(p, j, 0).start())
        pl.when(has_left)(lambda: gather(p, j, 1).start())
        gather(p, j, 2).start()

    @pl.loop(0, C)
    def _(s):
        k = jnp.where(s <= 2 * both, (s + 1) // 2, s - both)
        side = jnp.where((s <= 2 * both) & (s % 2 == 1), near, -near)
        b = p + side * k

        pl.when(outer & (s >= 1))(lambda: relay(s, 1))
        with jax.named_scope("await"):
            for j in range(S):
                gathered(b, j, 1 - c)
        norm(b)
        expand(s)
        pl.when(inner & (s >= 3))(lambda: relay(s, 1))
        pl.when((outer | (s >= 2)) & (s + 1 <= C - 1))(lambda: relay(s + 1, 0))
        pl.when(s == 3)(lambda: earlier())
        down(b, s)
        pl.when(s == 1)(lambda: early(0))

    late = C == 4
    for b in range(C):
        done = ((p == 1) & ((b <= C - 2) | late)) | ((p == 2) & (b == 1) & (C > 3))
        pl.when(inner & jnp.logical_not(done))(lambda: forward_right(b))
        done = ((p == C - 2) & ((b <= C - 2) | late)) | ((p == C - 3) & (b == 1) & (C > 3))
        pl.when(inner & jnp.logical_not(done))(lambda: forward_left(C - 1 - b))
    if late:
        pl.when(p == 1)(lambda: forward_right(C - 1))
        pl.when(p == C - 2)(lambda: forward_left(0))
    for b in range(C):
        final(jnp.where(leans_left, C - 1 - b, b))

    @jax.named_scope("drain")
    def drain(b):
        for j in range(S):
            pl.when((b <= p) & has_right)(lambda: gather(b, j, 0).wait_send())
            pl.when((b >= p) & has_left)(lambda: gather(b, j, 1).wait_send())
            gather(b, j, 2).wait_send()
        for d in range(C):
            to_peer(b, d).wait_send()
            pl.when(d != p)(lambda: to_right(b, d).wait_send())

    for b in range(C):
        drain(b)
    for b in range(C):
        store(b).wait()


def on_device(n, tokens, norm_gain, gate_weight, up_weight, down_weight):
    S = SUBS
    R, D = tokens.shape
    F = gate_weight.shape[1]
    C = n // 2
    T, W = 2 * R, D // n
    any_space, vmem = pl.BlockSpec(memory_space=pl.ANY), pl.BlockSpec(memory_space=pltpu.VMEM)
    dma = pltpu.SemaphoreType.DMA
    return pl.pallas_call(
        functools.partial(block_kernel, n),
        out_shape=jax.ShapeDtypeStruct((n * R, W), bf16),
        in_specs=[any_space, vmem, any_space, any_space, any_space],
        out_specs=any_space,
        scratch_shapes=[
            pltpu.VMEM((D, F), bf16),
            pltpu.VMEM((D, F), bf16),
            pltpu.VMEM((2, F, D // 2), bf16),
            pltpu.VMEM((C * T, D), bf16),
            pltpu.VMEM((T, D), bf16),
            pltpu.VMEM((T, F), bf16),
            pltpu.VMEM((C, T, W), f32),
            pltpu.VMEM((C, T, W), bf16),
            pltpu.VMEM((C, C, T, W), bf16),
            pltpu.VMEM((C, C, T, W), bf16),
            pltpu.VMEM((C, C, T, W), bf16),
            pltpu.VMEM((C, C + 1, T, W), bf16),
            pltpu.VMEM((2, T, W), bf16),
            pltpu.VMEM((C * T, W), f32),
            dma((4 + n,)),
            dma((S,)),
            dma((C, S, 2)),
            dma((3, C, S)),
            dma((C, C)),
            dma((C, C)),
            dma((C, C)),
            dma((C, C + 1)),
            dma((2,)),
            dma((C,)),
        ],
        compiler_params=pltpu.CompilerParams(collective_id=0, has_side_effects=True, vmem_limit_bytes=VMEM_LIMIT),
    )(tokens, norm_gain[None, :], gate_weight, up_weight, down_weight)


def solution(mesh):
    return jax.shard_map(
        functools.partial(on_device, mesh.shape["tensor"]),
        mesh=mesh,
        in_specs=(
            P(("dp", "tensor"), None),
            P(),
            P(None, "tensor"),
            P(None, "tensor"),
            P("tensor", None),
        ),
        out_specs=P("dp", "tensor"),
        check_vma=False,
    )
```

```python
import functools

import jax
import jax.numpy as jnp
from jax import lax
from jax.experimental import pallas as pl
from jax.experimental.pallas import tpu as pltpu
from jax.sharding import PartitionSpec as P

SUBS = 2
VMEM_LIMIT = 63963136
f32, bf16 = jnp.float32, jnp.bfloat16


def tile_of(F):
    return next(t for t in (256, 128) if F % t == 0)


def block_kernel(
    n, tok, gain, gw, uw, dw, out,
    gwv, uwv, dwv, every, normed, hidden, half, mine, theirs, peer, arrived, far,
    load_sem, own_sem, ag_recv, ag_send, peer_send, peer_recv, rs_send, rs_recv, far_recv,
):
    S = SUBS
    dp = lax.axis_index("dp")
    me = lax.axis_index("tensor")
    C = n // 2
    p, c = me // 2, me % 2
    R, D = tok.shape
    Rs = R // S
    T = 2 * R
    F = gwv.shape[1]
    W = D // n
    tile = tile_of(F)
    tiles = F // tile
    cuts = [0, (tiles + 1) // 2, tiles]
    partner = (dp, 2 * p + (1 - c))
    right = (dp, lax.rem(me + 2, n))
    left = (dp, lax.rem(me + n - 2, n))
    has_right, has_left = p < C - 1, p > 0
    inner = has_right & has_left
    leans_left = 2 * p < C - 1
    near = jnp.where(leans_left, -1, 1)
    both = jnp.where(leans_left, p, C - 1 - p)

    def rows_of(b, j, q):
        return pl.ds(pl.multiple_of(((b * S + j) * 2 + q) * Rs, Rs), Rs)

    def block_rows(b):
        return pl.ds(pl.multiple_of(b * T, T), T)

    def columns(t):
        return pl.ds(pl.multiple_of(t * W, W), W)

    own = [pltpu.make_async_copy(tok.at[pl.ds(j * Rs, Rs), :], every.at[rows_of(p, j, c), :], own_sem.at[j]) for j in range(S)]

    def load_wide(i):
        at = pl.ds(cuts[i] * tile, (cuts[i + 1] - cuts[i]) * tile)
        return (
            pltpu.make_async_copy(gw.at[:, at], gwv.at[:, at], load_sem.at[2 * i]),
            pltpu.make_async_copy(uw.at[:, at], uwv.at[:, at], load_sem.at[2 * i + 1]),
        )

    def load_down(q, d):
        return pltpu.make_async_copy(
            dw.at[:, columns(2 * d + q)], dwv.at[q, :, pl.ds(d * W, W)], load_sem.at[4 + C * q + d]
        )

    for copy in own:
        copy.start()

    barrier = pltpu.get_barrier_semaphore()

    def greet(device):
        pl.semaphore_signal(barrier, inc=1, device_id=device, device_id_type=pl.DeviceIdType.MESH)

    greet(partner)
    pl.when(has_right)(lambda: greet(right))
    pl.when(has_left)(lambda: greet(left))
    with jax.named_scope("own"):
        for copy in own:
            copy.wait()
    for i in range(2):
        for copy in load_wide(i):
            copy.start()
    with jax.named_scope("barrier"):
        pl.semaphore_wait(barrier, 1 + has_right.astype(jnp.int32) + has_left.astype(jnp.int32))

    def remote(src, dst, s, d, device):
        return pltpu.make_async_remote_copy(
            src_ref=src, dst_ref=dst, send_sem=s, recv_sem=d, device_id=device, device_id_type=pl.DeviceIdType.MESH
        )

    def gather(b, j, way):
        at = every.at[rows_of(b, j, c), :]
        return remote(at, at, ag_send.at[way, b, j], ag_recv.at[b, j, c], (right, left, partner)[way])

    def gathered(b, j, q):
        at = every.at[rows_of(b, j, q), :]
        remote(at, at, ag_send.at[2, b, j], ag_recv.at[b, j, q], partner).wait_recv()

    @jax.named_scope("relay")
    def relay(k, j):
        @pl.when(p - k >= 0)
        def _():
            gathered(p - k, j, c)
            pl.when(has_right)(lambda: gather(p - k, j, 0).start())
            gather(p - k, j, 2).start()

        @pl.when(p + k <= C - 1)
        def _():
            gathered(p + k, j, c)
            pl.when(has_left)(lambda: gather(p + k, j, 1).start())
            gather(p + k, j, 2).start()

    def to_peer(b, d):
        return remote(theirs.at[b, d], peer.at[b, d], peer_send.at[b, d], peer_recv.at[b, d], partner)

    def to_right(b, d):
        return remote(mine.at[b, d], arrived.at[b, d + 1], rs_send.at[b, d], rs_recv.at[b, d + 1], right)

    def to_left(b, d):
        return remote(mine.at[b, d], arrived.at[b, d], rs_send.at[b, d], rs_recv.at[b, d], left)

    def to_far(side, b, d):
        return remote(mine.at[b, d], far.at[side], rs_send.at[b, d], far_recv.at[side], (dp, 2 * d + c))

    def landed(b, slot):
        remote(arrived.at[b, slot], arrived.at[b, slot], rs_send.at[b, 0], rs_recv.at[b, slot], partner).wait_recv()

    def landed_far(side):
        remote(far.at[side], far.at[side], rs_send.at[0, 0], far_recv.at[side], partner).wait_recv()

    def straight_right(b, d):
        return (C > 2) & (b == C - 1) & (d == C - 1)

    def straight_left(b, d):
        return (C > 2) & (b == 0) & (d == 0)

    def first_send(b, d):
        straight = straight_right(b, d)
        pl.when((p == 0) & straight)(lambda: to_far(0, b, d).start())
        pl.when((d > p) & jnp.where(straight, p == 1, p == 0))(lambda: to_right(b, d).start())
        straight = straight_left(b, d)
        pl.when((p == C - 1) & straight)(lambda: to_far(1, b, d).start())
        pl.when((d < p) & jnp.where(straight, p == C - 2, p == C - 1))(lambda: to_left(b, d).start())

    def add_to_mine(b, d, slot):
        landed(b, slot)
        mine[b, d] = (mine[b, d].astype(f32) + arrived[b, slot].astype(f32)).astype(bf16)

    @jax.named_scope("right")
    def forward_right(b, targets=range(C - 1, 0, -1)):
        for d in targets:
            @pl.when((d > p) & jnp.logical_not((p == 1) & straight_right(b, d)))
            def _():
                add_to_mine(b, d, d + 1)
                to_right(b, d).start()

    @jax.named_scope("left")
    def forward_left(b, targets=range(C - 1)):
        for d in targets:
            @pl.when((d < p) & jnp.logical_not((p == C - 2) & straight_left(b, d)))
            def _():
                add_to_mine(b, d, d)
                to_left(b, d).start()

    def early(b, part):
        ahead = slice(0, 1) if part == 0 else slice(1, None)
        pl.when((p == 1) & has_right)(lambda: forward_right(b, range(C - 1, 0, -1)[ahead]))
        pl.when((p == C - 2) & has_left)(lambda: forward_left(C - 1 - b, range(C - 1)[ahead]))

    def earlier():
        pl.when((p == 2) & has_right)(lambda: forward_right(1))
        pl.when((p == C - 3) & has_left)(lambda: forward_left(C - 2))

    def pieces(b):
        for j in range(S):
            for q in range(2):
                yield pl.ds((j * 2 + q) * Rs, Rs), rows_of(b, j, q), pl.ds(pl.multiple_of((2 * b + q) * R + j * Rs, Rs), Rs)

    def add_to_out(b, ref):
        for at, _, to in pieces(b):
            out[to, :] += ref[at, :].astype(f32)

    @jax.named_scope("final")
    def final(b):
        @pl.when(has_left)
        def _():
            landed(b, p + 1)
            add_to_out(b, arrived.at[b, p + 1])

        @pl.when(has_right)
        def _():
            landed(b, p)
            add_to_out(b, arrived.at[b, p])

        @pl.when(straight_right(b, p))
        def _():
            landed_far(0)
            add_to_out(b, far.at[0])

        @pl.when(straight_left(b, p))
        def _():
            landed_far(1)
            add_to_out(b, far.at[1])

    @jax.named_scope("norm")
    def norm(b, j, q):
        wide = every[rows_of(b, j, q), :].astype(f32)
        scale = 1.0 / jnp.sqrt(jnp.mean(wide * wide, axis=1, keepdims=True) + 1e-05)
        normed[rows_of(0, j, q), :] = (wide * gain[...] * scale).astype(bf16)

    def expand(s):
        def part(i):
            for x in range(cuts[i], cuts[i + 1]):
                at = pl.ds(x * tile, tile)
                gate = jnp.dot(normed[...], gwv[:, at], preferred_element_type=f32)
                up = jnp.dot(normed[...], uwv[:, at], preferred_element_type=f32)
                hidden[:, at] = (jax.nn.silu(gate) * up).astype(bf16)

        @pl.when(s == 0)
        def _():
            with jax.named_scope("load"):
                for copy in load_wide(0):
                    copy.wait()
                for q in range(2):
                    for d in range(C):
                        load_down(jnp.where(c == 0, 1 - q, q), d).start()

        with jax.named_scope("expand0"):
            part(0)

        @pl.when(s == 0)
        def _():
            with jax.named_scope("load"):
                for copy in load_wide(1):
                    copy.wait()

        with jax.named_scope("expand1"):
            part(1)

    def down(b, s):
        far_block = jnp.where(leans_left, (p == 0) & (b == C - 1), (p == C - 1) & (b == 0)) & (C > 2)

        def dest(i):
            i = jnp.where(far_block, 1 - i, i) if i < 2 else i
            return jnp.where(leans_left, C - 1 - i, i)

        def product(q, d):
            return jnp.dot(hidden[...], dwv[q, :, pl.ds(pl.multiple_of(d * W, W), W)], preferred_element_type=f32)

        @pl.when(s == 0)
        def _():
            with jax.named_scope("load"):
                for d in range(C):
                    load_down(1 - c, d).wait()

        def give(at):
            with jax.named_scope("down0"):
                for i in at:
                    theirs[b, dest(i)] = product(1 - c, dest(i)).astype(bf16)
            for i in at:
                to_peer(b, dest(i)).start()

        def take(at):
            with jax.named_scope("down1"):
                for i in at:
                    half[dest(i)] = product(c, dest(i))
            for i in at:
                d = dest(i)
                with jax.named_scope("peer"):
                    to_peer(b, d).wait_recv()
                mine[b, d] = (half[d] + peer[b, d].astype(f32)).astype(bf16)
                first_send(b, d)

        give(range(1))
        give(range(1, C))

        @pl.when(s == 0)
        def _():
            with jax.named_scope("load"):
                for d in range(C):
                    load_down(c, d).wait()

        take(range(1))
        take(range(1, C))

        for at, rows, to in pieces(b):
            out[to, :] = every[rows, columns(me)].astype(f32) + mine[b, p, at, :].astype(f32)

    for j in range(S):
        pl.when(has_right)(lambda: gather(p, j, 0).start())
        pl.when(has_left)(lambda: gather(p, j, 1).start())
        gather(p, j, 2).start()

    @pl.loop(0, C)
    def _(s):
        k = jnp.where(s <= 2 * both, (s + 1) // 2, s - both)
        side = jnp.where((s <= 2 * both) & (s % 2 == 1), near, -near)
        b = p + side * k

        def other(j):
            with jax.named_scope("await"):
                gathered(b, j, 1 - c)

        for j in range(S - 1):
            other(j)
            for q in range(2):
                norm(b, j, q)
        pl.when(s >= 1)(lambda: relay(s, S - 1))
        norm(b, S - 1, c)
        other(S - 1)
        norm(b, S - 1, 1 - c)
        expand(s)
        pl.when(s + 1 <= C - 1)(lambda: relay(s + 1, 0))
        pl.when(s >= 2)(lambda: early(s - 1, 0))
        pl.when(s == 3)(lambda: earlier())
        down(b, s)
        pl.when(s == 1)(lambda: early(0, 0))
        pl.when((s >= 1) & (s <= C - 2))(lambda: early(s - 1, 1))

    late = C == 4
    for b in range(C):
        done = ((p == 1) & ((b <= C - 2) | late)) | ((p == 2) & (b == 1) & (C > 3))
        pl.when(inner & jnp.logical_not(done))(lambda: forward_right(b))
        done = ((p == C - 2) & ((b <= C - 2) | late)) | ((p == C - 3) & (b == 1) & (C > 3))
        pl.when(inner & jnp.logical_not(done))(lambda: forward_left(C - 1 - b))
        if b == 0:
            early(C - 2, 1)
    if late:
        pl.when(p == 1)(lambda: forward_right(C - 1))
        pl.when(p == C - 2)(lambda: forward_left(0))
    for b in range(C):
        final(jnp.where(leans_left, C - 1 - b, b))

    @jax.named_scope("drain")
    def drain(b):
        for j in range(S):
            pl.when((b <= p) & has_right)(lambda: gather(b, j, 0).wait_send())
            pl.when((b >= p) & has_left)(lambda: gather(b, j, 1).wait_send())
            gather(b, j, 2).wait_send()
        for d in range(C):
            to_peer(b, d).wait_send()
            pl.when(d != p)(lambda: to_right(b, d).wait_send())

    for b in range(C):
        drain(b)


def on_device(n, tokens, norm_gain, gate_weight, up_weight, down_weight):
    S = SUBS
    R, D = tokens.shape
    F = gate_weight.shape[1]
    C = n // 2
    T, W = 2 * R, D // n
    any_space, vmem = pl.BlockSpec(memory_space=pl.ANY), pl.BlockSpec(memory_space=pltpu.VMEM)
    dma = pltpu.SemaphoreType.DMA
    mixed = pl.pallas_call(
        functools.partial(block_kernel, n),
        out_shape=pltpu.VMEM((n * R, W), f32),
        in_specs=[any_space, vmem, any_space, any_space, any_space],
        out_specs=vmem,
        scratch_shapes=[
            pltpu.VMEM((D, F), bf16),
            pltpu.VMEM((D, F), bf16),
            pltpu.VMEM((2, F, D // 2), bf16),
            pltpu.VMEM((C * T, D), bf16),
            pltpu.VMEM((T, D), bf16),
            pltpu.VMEM((T, F), bf16),
            pltpu.VMEM((C, T, W), f32),
            pltpu.VMEM((C, C, T, W), bf16),
            pltpu.VMEM((C, C, T, W), bf16),
            pltpu.VMEM((C, C, T, W), bf16),
            pltpu.VMEM((C, C + 1, T, W), bf16),
            pltpu.VMEM((2, T, W), bf16),
            dma((4 + n,)),
            dma((S,)),
            dma((C, S, 2)),
            dma((3, C, S)),
            dma((C, C)),
            dma((C, C)),
            dma((C, C)),
            dma((C, C + 1)),
            dma((2,)),
        ],
        compiler_params=pltpu.CompilerParams(collective_id=0, has_side_effects=True, vmem_limit_bytes=VMEM_LIMIT),
    )(tokens, norm_gain[None, :], gate_weight, up_weight, down_weight)
    return mixed.astype(bf16)


def solution(mesh):
    return jax.shard_map(
        functools.partial(on_device, mesh.shape["tensor"]),
        mesh=mesh,
        in_specs=(
            P(("dp", "tensor"), None),
            P(),
            P(None, "tensor"),
            P(None, "tensor"),
            P("tensor", None),
        ),
        out_specs=P("dp", "tensor"),
        check_vma=False,
    )
```

```python
import functools

import jax
import jax.numpy as jnp
from jax import lax
from jax.experimental import pallas as pl
from jax.experimental.pallas import tpu as pltpu
from jax.sharding import PartitionSpec as P

SUBS = 2
VMEM_LIMIT = 63963136
f32, bf16 = jnp.float32, jnp.bfloat16


def tile_of(F):
    return next(t for t in (256, 128) if F % t == 0)


def block_kernel(
    n, tok, gain, gw, uw, dw, out,
    wide, dwv, gainv, every, normed, hidden, other, half, mine, arrived, far,
    load_sem, own_sem, ag_recv, ag_send, pair_send, pair_recv, down_send, down_recv, rs_send, rs_recv, far_recv,
):
    S = SUBS
    dp = lax.axis_index("dp")
    me = lax.axis_index("tensor")
    C = n // 2
    p, c = me // 2, me % 2
    R, D = tok.shape
    Rs = R // S
    T = 2 * R
    F = wide.shape[2]
    W = D // n
    tile = tile_of(F)
    tiles = F // tile
    cuts = [0, (tiles + 1) // 2, tiles]
    partner = (dp, 2 * p + (1 - c))
    right = (dp, lax.rem(me + 2, n))
    left = (dp, lax.rem(me + n - 2, n))
    has_right, has_left = p < C - 1, p > 0
    inner = has_right & has_left
    leans_left = 2 * p < C - 1
    near = jnp.where(leans_left, -1, 1)
    both = jnp.where(leans_left, p, C - 1 - p)

    def rows_of(b, j, q):
        return pl.ds(pl.multiple_of(((b * S + j) * 2 + q) * Rs, Rs), Rs)

    def block_rows(b):
        return pl.ds(pl.multiple_of(b * T, T), T)

    def columns(t):
        return pl.ds(pl.multiple_of(t * W, W), W)

    own = [pltpu.make_async_copy(tok.at[pl.ds(j * Rs, Rs), :], every.at[rows_of(p, j, c), :], own_sem.at[0]) for j in range(S)]
    gain_copy = pltpu.make_async_copy(gain, gainv, own_sem.at[1])

    def load_wide(i):
        at = pl.ds(cuts[i] * tile, (cuts[i + 1] - cuts[i]) * tile)
        return [pltpu.make_async_copy((gw, uw)[x].at[:, at], wide.at[x, :, at], load_sem.at[i]) for x in range(2)]

    def load_down(d):
        return pltpu.make_async_copy(dw.at[:, columns(2 * d + c)], dwv.at[0, :, pl.ds(d * W, W)], load_sem.at[2])

    def all_of(ref, sem):
        pltpu.make_async_copy(ref, ref, sem).wait()

    def wide_loaded(i):
        all_of(wide.at[:, :, pl.ds(cuts[i] * tile, (cuts[i + 1] - cuts[i]) * tile)], load_sem.at[i])

    for copy in own:
        copy.start()
    gain_copy.start()

    barrier = pltpu.get_barrier_semaphore()

    def greet(device):
        pl.semaphore_signal(barrier, inc=1, device_id=device, device_id_type=pl.DeviceIdType.MESH)

    greet(partner)
    pl.when(has_right)(lambda: greet(right))
    pl.when(has_left)(lambda: greet(left))
    with jax.named_scope("own"):
        all_of(every.at[pl.ds(0, R), :], own_sem.at[0])
    for i in range(2):
        for copy in load_wide(i):
            copy.start()
    with jax.named_scope("barrier"):
        pl.semaphore_wait(barrier, 1 + has_right.astype(jnp.int32) + has_left.astype(jnp.int32))

    def remote(src, dst, s, d, device):
        return pltpu.make_async_remote_copy(
            src_ref=src, dst_ref=dst, send_sem=s, recv_sem=d, device_id=device, device_id_type=pl.DeviceIdType.MESH
        )

    def gather(b, j, way):
        at = every.at[rows_of(b, j, c), :]
        return remote(at, at, ag_send.at[way], ag_recv.at[b, j, c], (right, left, partner)[way])

    def gathered(b, j, q):
        at = every.at[rows_of(b, j, q), :]
        remote(at, at, ag_send.at[2], ag_recv.at[b, j, q], partner).wait_recv()

    @jax.named_scope("relay")
    def relay(k, j):
        @pl.when(p - k >= 0)
        def _():
            gathered(p - k, j, c)
            pl.when(has_right)(lambda: gather(p - k, j, 0).start())
            gather(p - k, j, 2).start()

        @pl.when(p + k <= C - 1)
        def _():
            gathered(p + k, j, c)
            pl.when(has_left)(lambda: gather(p + k, j, 1).start())
            gather(p + k, j, 2).start()

    def share_down(d):
        return remote(dw.at[:, columns(2 * d + 1 - c)], dwv.at[1, :, pl.ds(d * W, W)], down_send, down_recv, partner)

    def share_hidden(s, i):
        at = pl.ds(cuts[i] * tile, (cuts[i + 1] - cuts[i]) * tile)
        return remote(hidden.at[s % 2, :, at], other.at[s % 2, :, at], pair_send, pair_recv.at[s % 2, i], partner)

    def to_right(b, d):
        return remote(mine.at[b, d], arrived.at[b, d + 1], rs_send, rs_recv.at[b, d + 1], right)

    def to_left(b, d):
        return remote(mine.at[b, d], arrived.at[b, d], rs_send, rs_recv.at[b, d], left)

    def to_far(b, d):
        return remote(mine.at[b, d], far, rs_send, far_recv, (dp, 2 * d + c))

    def landed(b, slot):
        remote(arrived.at[b, slot], arrived.at[b, slot], rs_send, rs_recv.at[b, slot], partner).wait_recv()

    def landed_far():
        remote(far, far, rs_send, far_recv, partner).wait_recv()

    def straight_right(b, d):
        return (C > 2) & (b == C - 1) & (d == C - 1)

    def straight_left(b, d):
        return (C > 2) & (b == 0) & (d == 0)

    def first_send(b, d):
        straight = straight_right(b, d)
        pl.when((p == 0) & straight)(lambda: to_far(b, d).start())
        pl.when((d > p) & jnp.where(straight, p == 1, p == 0))(lambda: to_right(b, d).start())
        straight = straight_left(b, d)
        pl.when((p == C - 1) & straight)(lambda: to_far(b, d).start())
        pl.when((d < p) & jnp.where(straight, p == C - 2, p == C - 1))(lambda: to_left(b, d).start())

    def add_to_mine(b, d, slot):
        landed(b, slot)
        mine[b, d] = (mine[b, d].astype(f32) + arrived[b, slot].astype(f32)).astype(bf16)

    @jax.named_scope("right")
    def forward_right(b, targets=range(C - 1, 0, -1)):
        for d in targets:
            @pl.when((d > p) & jnp.logical_not((p == 1) & straight_right(b, d)))
            def _():
                add_to_mine(b, d, d + 1)
                to_right(b, d).start()

    @jax.named_scope("left")
    def forward_left(b, targets=range(C - 1)):
        for d in targets:
            @pl.when((d < p) & jnp.logical_not((p == C - 2) & straight_left(b, d)))
            def _():
                add_to_mine(b, d, d)
                to_left(b, d).start()

    def early(b, part):
        ahead = slice(0, 1) if part == 0 else slice(1, None)
        pl.when((p == 1) & has_right)(lambda: forward_right(b, range(C - 1, 0, -1)[ahead]))
        pl.when((p == C - 2) & has_left)(lambda: forward_left(C - 1 - b, range(C - 1)[ahead]))

    def earlier():
        pl.when((p == 2) & has_right)(lambda: forward_right(1))
        pl.when((p == C - 3) & has_left)(lambda: forward_left(C - 2))

    def pieces(b):
        for j in range(S):
            for q in range(2):
                yield pl.ds((j * 2 + q) * Rs, Rs), rows_of(b, j, q), pl.ds(pl.multiple_of((2 * b + q) * R + j * Rs, Rs), Rs)

    def add_to_out(b, ref):
        for at, _, to in pieces(b):
            out[to, :] += ref[at, :].astype(f32)

    @jax.named_scope("final")
    def final(b):
        @pl.when(has_left)
        def _():
            landed(b, p + 1)
            add_to_out(b, arrived.at[b, p + 1])

        @pl.when(has_right)
        def _():
            landed(b, p)
            add_to_out(b, arrived.at[b, p])

        @pl.when(straight_right(b, p) | straight_left(b, p))
        def _():
            landed_far()
            add_to_out(b, far)

    @jax.named_scope("norm")
    def norm(b, j, q):
        rows = every[rows_of(b, j, q), :].astype(f32)
        scale = 1.0 / jnp.sqrt(jnp.mean(rows * rows, axis=1, keepdims=True) + 1e-05)
        normed[rows_of(0, j, q), :] = (rows * gainv[...] * scale).astype(bf16)

    def expand(s):
        def part(i):
            for x in range(cuts[i], cuts[i + 1]):
                at = pl.ds(x * tile, tile)
                gate = jnp.dot(normed[...], wide[0, :, at], preferred_element_type=f32)
                up = jnp.dot(normed[...], wide[1, :, at], preferred_element_type=f32)
                hidden[s % 2, :, at] = (jax.nn.silu(gate) * up).astype(bf16)

        @pl.when(s == 0)
        def _():
            with jax.named_scope("load"):
                wide_loaded(0)
                for d in range(C):
                    load_down(d).start()

        with jax.named_scope("expand0"):
            part(0)
        share_hidden(s, 0).start()

        @pl.when(s == 0)
        def _():
            with jax.named_scope("load"):
                wide_loaded(1)

        with jax.named_scope("expand1"):
            part(1)
        share_hidden(s, 1).start()

    def down(b, s):
        far_block = jnp.where(leans_left, (p == 0) & (b == C - 1), (p == C - 1) & (b == 0)) & (C > 2)

        def dest(i):
            i = jnp.where(far_block, 1 - i, i) if i < 2 else i
            return jnp.where(leans_left, C - 1 - i, i)

        def product(of, x, d):
            weight = dwv[x, :, pl.ds(pl.multiple_of(d * W, W), W)]
            return jnp.dot(of[s % 2], weight, preferred_element_type=f32)

        @pl.when(s == 0)
        def _():
            with jax.named_scope("load"):
                all_of(dwv.at[0], load_sem.at[2])

        with jax.named_scope("down0"):
            for d in range(C):
                half[d] = product(hidden, 0, d)

        @pl.when(s == 0)
        def _():
            with jax.named_scope("load"):
                remote(dwv.at[1], dwv.at[1], down_send, down_recv, partner).wait_recv()

        with jax.named_scope("peer"):
            for i in range(2):
                share_hidden(s, i).wait_recv()
        for at in (range(1), range(1, C)):
            with jax.named_scope("down1"):
                for i in at:
                    d = dest(i)
                    mine[b, d] = (half[d] + product(other, 1, d)).astype(bf16)
            for i in at:
                first_send(b, dest(i))
        all_of(hidden.at[s % 2], pair_send)

        for at, rows, to in pieces(b):
            out[to, :] = every[rows, columns(me)].astype(f32) + mine[b, p, at, :].astype(f32)

    for j in range(S):
        pl.when(has_right)(lambda: gather(p, j, 0).start())
        pl.when(has_left)(lambda: gather(p, j, 1).start())
        gather(p, j, 2).start()
    for d in range(C):
        share_down(d).start()

    @pl.loop(0, C)
    def _(s):
        k = jnp.where(s <= 2 * both, (s + 1) // 2, s - both)
        side = jnp.where((s <= 2 * both) & (s % 2 == 1), near, -near)
        b = p + side * k

        def other(j):
            with jax.named_scope("await"):
                gathered(b, j, 1 - c)

        for j in range(S - 1):
            other(j)
            if j == 0:
                pl.when(s == 0)(lambda: gain_copy.wait())
            for q in range(2):
                norm(b, j, q)
        pl.when(s >= 1)(lambda: relay(s, S - 1))
        norm(b, S - 1, c)
        other(S - 1)
        norm(b, S - 1, 1 - c)
        expand(s)
        pl.when(s + 1 <= C - 1)(lambda: relay(s + 1, 0))
        pl.when(s >= 2)(lambda: early(s - 1, 0))
        pl.when(s == 3)(lambda: earlier())
        down(b, s)
        pl.when(s == 1)(lambda: early(0, 0))
        pl.when((s >= 1) & (s <= C - 2))(lambda: early(s - 1, 1))

    late = C == 4
    for b in range(C):
        done = ((p == 1) & ((b <= C - 2) | late)) | ((p == 2) & (b == 1) & (C > 3))
        pl.when(inner & jnp.logical_not(done))(lambda: forward_right(b))
        done = ((p == C - 2) & ((b <= C - 2) | late)) | ((p == C - 3) & (b == 1) & (C > 3))
        pl.when(inner & jnp.logical_not(done))(lambda: forward_left(C - 1 - b))
        if b == 0:
            early(C - 2, 1)
    if late:
        pl.when(p == 1)(lambda: forward_right(C - 1))
        pl.when(p == C - 2)(lambda: forward_left(0))
    for b in range(C):
        final(jnp.where(leans_left, C - 1 - b, b))

    with jax.named_scope("drain"):
        for x in range(C):
            pl.when((p == x) & has_right)(lambda: all_of(every.at[pl.ds(0, (x + 1) * R), :], ag_send.at[0]))
            pl.when((p == x) & has_left)(lambda: all_of(every.at[pl.ds(0, (C - x) * R), :], ag_send.at[1]))
        all_of(every.at[pl.ds(0, C * R), :], ag_send.at[2])
        all_of(dwv.at[1], down_send)
        all_of(mine.at[:, pl.ds(0, C - 1)], rs_send)


def on_device(n, tokens, norm_gain, gate_weight, up_weight, down_weight):
    S = SUBS
    R, D = tokens.shape
    F = gate_weight.shape[1]
    C = n // 2
    T, W = 2 * R, D // n
    any_space, vmem = pl.BlockSpec(memory_space=pl.ANY), pl.BlockSpec(memory_space=pltpu.VMEM)
    dma = pltpu.SemaphoreType.DMA
    mixed = pl.pallas_call(
        functools.partial(block_kernel, n),
        out_shape=pltpu.VMEM((n * R, W), f32),
        in_specs=[any_space] * 5,
        out_specs=vmem,
        scratch_shapes=[
            pltpu.VMEM((2, D, F), bf16),
            pltpu.VMEM((2, F, D // 2), bf16),
            pltpu.VMEM((1, D), f32),
            pltpu.VMEM((C * T, D), bf16),
            pltpu.VMEM((T, D), bf16),
            pltpu.VMEM((2, T, F), bf16),
            pltpu.VMEM((2, T, F), bf16),
            pltpu.VMEM((C, T, W), f32),
            pltpu.VMEM((C, C, T, W), bf16),
            pltpu.VMEM((C, C + 1, T, W), bf16),
            pltpu.VMEM((T, W), bf16),
            dma((3,)),
            dma((2,)),
            dma((C, S, 2)),
            dma((3,)),
            dma,
            dma((2, 2)),
            dma,
            dma,
            dma,
            dma((C, C + 1)),
            dma,
        ],
        compiler_params=pltpu.CompilerParams(collective_id=0, has_side_effects=True, vmem_limit_bytes=VMEM_LIMIT),
    )(tokens, norm_gain[None, :], gate_weight, up_weight, down_weight)
    return mixed.astype(bf16)


def solution(mesh):
    return jax.shard_map(
        functools.partial(on_device, mesh.shape["tensor"]),
        mesh=mesh,
        in_specs=(
            P(("dp", "tensor"), None),
            P(),
            P(None, "tensor"),
            P(None, "tensor"),
            P("tensor", None),
        ),
        out_specs=P("dp", "tensor"),
        check_vma=False,
    )
```

```python
import functools

import jax
import jax.numpy as jnp
from jax import lax
from jax.experimental import pallas as pl
from jax.experimental.pallas import tpu as pltpu
from jax.sharding import PartitionSpec as P

SUBS = 2
VMEM_LIMIT = 63963136
f32, bf16 = jnp.float32, jnp.bfloat16


def tile_of(F):
    return next(t for t in (256, 128) if F % t == 0)


def block_kernel(
    n, tok, gain, gw, uw, dw, out,
    wide, dwv, gainv, every, normed, sums, partial, hidden, other, half, mine, arrived, far, acc,
    load_sem, own_sem, ag_recv, ag_send, pair_send, pair_recv, down_send, down_recv, rs_send, rs_recv, far_recv,
):
    S = SUBS
    dp = lax.axis_index("dp")
    me = lax.axis_index("tensor")
    C = n // 2
    p, c = me // 2, me % 2
    R, D = tok.shape
    Dc = D // S
    T = 2 * R
    F = wide.shape[2]
    W = D // n
    tile = tile_of(F)
    tiles = F // tile
    cuts = [0, (tiles + 1) // 2, tiles]
    partner = (dp, 2 * p + (1 - c))
    right = (dp, lax.rem(me + 2, n))
    left = (dp, lax.rem(me + n - 2, n))
    has_right, has_left = p < C - 1, p > 0
    inner = has_right & has_left
    outer = jnp.logical_not(inner)
    late = C == 4
    leans_left = 2 * p < C - 1
    near = jnp.where(leans_left, -1, 1)
    both = jnp.where(leans_left, p, C - 1 - p)

    def rows_of(b, q):
        return pl.ds(pl.multiple_of((b * 2 + q) * R, R), R)

    def features(j):
        return pl.ds(j * Dc, Dc)

    def block_rows(b):
        return pl.ds(pl.multiple_of(b * T, T), T)

    def columns(t):
        return pl.ds(pl.multiple_of(t * W, W), W)

    own = [pltpu.make_async_copy(tok.at[:, features(j)], every.at[rows_of(p, c), features(j)], own_sem.at[0]) for j in range(S)]
    gain_copy = pltpu.make_async_copy(gain, gainv, own_sem.at[1])

    def load_wide(j):
        return [pltpu.make_async_copy((gw, uw)[x].at[features(j), :], wide.at[x, features(j), :], load_sem.at[j]) for x in range(2)]

    def load_down(d):
        return pltpu.make_async_copy(dw.at[:, columns(2 * d + c)], dwv.at[0, :, pl.ds(d * W, W)], load_sem.at[S])

    def all_of(ref, sem):
        pltpu.make_async_copy(ref, ref, sem).wait()

    def wide_loaded(i):
        all_of(wide.at[:, features(i), :], load_sem.at[i])

    for copy in own:
        copy.start()
    gain_copy.start()

    barrier = pltpu.get_barrier_semaphore()

    def greet(device):
        pl.semaphore_signal(barrier, inc=1, device_id=device, device_id_type=pl.DeviceIdType.MESH)

    greet(partner)
    pl.when(has_right)(lambda: greet(right))
    pl.when(has_left)(lambda: greet(left))
    with jax.named_scope("own"):
        all_of(every.at[pl.ds(0, R), :], own_sem.at[0])
    for i in range(S):
        for copy in load_wide(i):
            copy.start()
    with jax.named_scope("barrier"):
        pl.semaphore_wait(barrier, 1 + has_right.astype(jnp.int32) + has_left.astype(jnp.int32))

    def remote(src, dst, s, d, device):
        return pltpu.make_async_remote_copy(
            src_ref=src, dst_ref=dst, send_sem=s, recv_sem=d, device_id=device, device_id_type=pl.DeviceIdType.MESH
        )

    def gather(b, j, way):
        at = every.at[rows_of(b, c), features(j)]
        return remote(at, at, ag_send.at[way], ag_recv.at[b, j, c], (right, left, partner)[way])

    def gathered(b, j, q):
        at = every.at[rows_of(b, q), features(j)]
        remote(at, at, ag_send.at[2], ag_recv.at[b, j, q], partner).wait_recv()

    @jax.named_scope("relay")
    def relay(k, j):
        @pl.when(p - k >= 0)
        def _():
            gathered(p - k, j, c)
            pl.when(has_right)(lambda: gather(p - k, j, 0).start())
            gather(p - k, j, 2).start()

        @pl.when(p + k <= C - 1)
        def _():
            gathered(p + k, j, c)
            pl.when(has_left)(lambda: gather(p + k, j, 1).start())
            gather(p + k, j, 2).start()

    def share_down(d):
        return remote(dw.at[:, columns(2 * d + 1 - c)], dwv.at[1, :, pl.ds(d * W, W)], down_send, down_recv, partner)

    def share_hidden(s, i):
        at = pl.ds(cuts[i] * tile, (cuts[i + 1] - cuts[i]) * tile)
        return remote(hidden.at[s % 2, :, at], other.at[s % 2, :, at], pair_send, pair_recv.at[s % 2, i], partner)

    def to_right(b, d):
        return remote(mine.at[b, d], arrived.at[b, d + 1], rs_send, rs_recv.at[b, d + 1], right)

    def to_left(b, d):
        return remote(mine.at[b, d], arrived.at[b, d], rs_send, rs_recv.at[b, d], left)

    def to_far(b, d):
        return remote(mine.at[b, d], far, rs_send, far_recv, (dp, 2 * d + c))

    def landed(b, slot):
        remote(arrived.at[b, slot], arrived.at[b, slot], rs_send, rs_recv.at[b, slot], partner).wait_recv()

    def landed_far():
        remote(far, far, rs_send, far_recv, partner).wait_recv()

    def straight_right(b, d):
        return (C > 2) & (b == C - 1) & (d == C - 1)

    def straight_left(b, d):
        return (C > 2) & (b == 0) & (d == 0)

    def first_send(b, d):
        straight = straight_right(b, d)
        pl.when((p == 0) & straight)(lambda: to_far(b, d).start())
        pl.when((d > p) & jnp.where(straight, p == 1, p == 0))(lambda: to_right(b, d).start())
        straight = straight_left(b, d)
        pl.when((p == C - 1) & straight)(lambda: to_far(b, d).start())
        pl.when((d < p) & jnp.where(straight, p == C - 2, p == C - 1))(lambda: to_left(b, d).start())

    def add_to_mine(b, d, slot):
        landed(b, slot)
        mine[b, d] = (mine[b, d].astype(f32) + arrived[b, slot].astype(f32)).astype(bf16)

    @jax.named_scope("right")
    def forward_right(b, targets=range(C - 1, 0, -1)):
        for d in targets:
            @pl.when((d > p) & jnp.logical_not((p == 1) & straight_right(b, d)))
            def _():
                add_to_mine(b, d, d + 1)
                to_right(b, d).start()

    @jax.named_scope("left")
    def forward_left(b, targets=range(C - 1)):
        for d in targets:
            @pl.when((d < p) & jnp.logical_not((p == C - 2) & straight_left(b, d)))
            def _():
                add_to_mine(b, d, d)
                to_left(b, d).start()

    def early_right(b, part):
        ahead = slice(0, 1) if part == 0 else slice(1, None)
        pl.when((p == 1) & has_right)(lambda: forward_right(b, range(C - 1, 0, -1)[ahead]))

    def early_left(b, part):
        ahead = slice(0, 1) if part == 0 else slice(1, None)
        pl.when((p == C - 2) & has_left)(lambda: forward_left(C - 1 - b, range(C - 1)[ahead]))

    def early(b, part):
        early_right(b, part)
        early_left(b, part)

    def earlier():
        pl.when((p == 2) & has_right)(lambda: forward_right(1))
        pl.when((p == C - 3) & has_left)(lambda: forward_left(C - 2))

    def add_to_out(b, ref):
        acc[block_rows(b), :] += ref[...].astype(f32)

    @jax.named_scope("final")
    def final(b):
        @pl.when(has_left)
        def _():
            landed(b, p + 1)
            add_to_out(b, arrived.at[b, p + 1])

        @pl.when(has_right)
        def _():
            landed(b, p)
            add_to_out(b, arrived.at[b, p])

        @pl.when(straight_right(b, p) | straight_left(b, p))
        def _():
            landed_far()
            add_to_out(b, far)

        out[block_rows(b), :] = acc[block_rows(b), :].astype(bf16)

    @jax.named_scope("norm")
    def prepare(b, j, q):
        rows = every[rows_of(b, q), features(j)].astype(f32)
        at = rows_of(0, q)
        sums[j, at, :] = jnp.broadcast_to(jnp.sum(rows * rows, axis=1, keepdims=True), (R, 128))
        normed[at, features(j)] = (rows * gainv[:, features(j)]).astype(bf16)

    def expand(b, s, k):
        def other_rows(j):
            with jax.named_scope("await"):
                gathered(b, j, 1 - c)

        def products(x, j):
            at = pl.ds(x * tile, tile)
            return [jnp.dot(normed[:, features(j)], wide[y, features(j), at], preferred_element_type=f32) for y in range(2)]

        pl.when(s == 0)(lambda: gain_copy.wait())
        for j in range(S - 1):
            prepare(b, j, c)
            other_rows(j)
            prepare(b, j, 1 - c)
            if j == S - 2:
                pl.when(inner & (s >= 1) & (k == s))(lambda: relay(s, S - 1))

            @pl.when(s == 0)
            def _():
                with jax.named_scope("load"):
                    wide_loaded(j)
                    if j == 0:
                        for d in range(C):
                            load_down(d).start()

            with jax.named_scope("expand0"):
                for x in range(tiles):
                    at = pl.ds(x * tile, tile)
                    for y, product in enumerate(products(x, j)):
                        partial[y, :, at] = product if j == 0 else partial[y, :, at] + product
        pl.when(outer & (s >= 1))(lambda: relay(s, S - 1))
        prepare(b, S - 1, c)
        other_rows(S - 1)
        prepare(b, S - 1, 1 - c)

        @pl.when(s == 0)
        def _():
            with jax.named_scope("load"):
                wide_loaded(S - 1)

        def part(i):
            scale = 1.0 / jnp.sqrt(sum(sums[j] for j in range(S)) / D + 1e-05)
            scale = jnp.concatenate([scale] * (tile // 128), axis=1)
            for x in range(cuts[i], cuts[i + 1]):
                at = pl.ds(x * tile, tile)
                gate, up = [(partial[y, :, at] + product) * scale for y, product in enumerate(products(x, S - 1))]
                hidden[s % 2, :, at] = (jax.nn.silu(gate) * up).astype(bf16)

        with jax.named_scope("expand1"):
            part(0)
        share_hidden(s, 0).start()
        pl.when(inner & (s >= 2) & (k != s))(lambda: relay(s, S - 1))
        with jax.named_scope("expand2"):
            part(1)
        share_hidden(s, 1).start()

    def down(b, s):
        turned = (p == 1) & (b == C - 1) if late else p < 0
        far_block = jnp.where(leans_left, (p == 0) & (b == C - 1), (p == C - 1) & (b == 0)) & (C > 2)

        def dest(i):
            i = jnp.where(far_block, 1 - i, i) if i < 2 else i
            return jnp.where(leans_left & jnp.logical_not(turned), C - 1 - i, i)

        def product(of, x, d):
            weight = dwv[x, :, pl.ds(pl.multiple_of(d * W, W), W)]
            return jnp.dot(of[s % 2], weight, preferred_element_type=f32)

        @pl.when(s == 0)
        def _():
            with jax.named_scope("load"):
                all_of(dwv.at[0], load_sem.at[S])

        with jax.named_scope("down0"):
            for d in range(C):
                half[d] = product(hidden, 0, d)

        @pl.when(s == 0)
        def _():
            with jax.named_scope("load"):
                remote(dwv.at[1], dwv.at[1], down_send, down_recv, partner).wait_recv()

        pl.when(outer & (s >= 1) & (s + 1 <= C - 1))(lambda: relay(s + 1, 0))
        pl.when(s >= 2)(lambda: early_right(s - 1, 0))
        with jax.named_scope("peer"):
            for i in range(2):
                share_hidden(s, i).wait_recv()
        for at in (range(1), range(1, C)):
            with jax.named_scope("down1"):
                for i in at:
                    d = dest(i)
                    mine[b, d] = (half[d] + product(other, 1, d)).astype(bf16)
            for i in at:
                first_send(b, dest(i))
            if late and len(at) == 1:
                pl.when(turned)(lambda: forward_left(C - 1))
        all_of(hidden.at[s % 2], pair_send)

        acc[block_rows(b), :] = every[block_rows(b), columns(me)].astype(f32) + mine[b, p].astype(f32)

    for j in range(S):
        pl.when(has_right)(lambda: gather(p, j, 0).start())
        pl.when(has_left)(lambda: gather(p, j, 1).start())
        gather(p, j, 2).start()
    for d in range(C):
        share_down(d).start()

    @pl.loop(0, C)
    def _(s):
        k = jnp.where(s <= 2 * both, (s + 1) // 2, s - both)
        side = jnp.where((s <= 2 * both) & (s % 2 == 1), near, -near)
        b = p + side * k

        def other_rows(j):
            with jax.named_scope("await"):
                gathered(b, j, 1 - c)

        expand(b, s, k)
        pl.when((inner | (s == 0)) & (s + 1 <= C - 1))(lambda: relay(s + 1, 0))
        pl.when(s >= 2)(lambda: early_left(s - 1, 0))
        pl.when(s == 3)(lambda: earlier())
        down(b, s)
        pl.when(s == 1)(lambda: early(0, 0))
        pl.when((s >= 1) & (s <= C - 2))(lambda: early(s - 1, 1))

    for b in range(C):
        done = ((p == 1) & ((b <= C - 2) | late)) | ((p == 2) & (b == 1) & (C > 3))
        pl.when(inner & jnp.logical_not(done))(lambda: forward_right(b))
        done = ((p == C - 2) & ((b <= C - 2) | late)) | ((p == C - 3) & ((b == 1) & (C > 3) | (b == 0) & late))
        pl.when(inner & jnp.logical_not(done))(lambda: forward_left(C - 1 - b))
        if b == 0:
            early(C - 2, 1)
    if late:
        pl.when(p == 1)(lambda: forward_right(C - 1))
        pl.when(p == C - 2)(lambda: forward_left(0))
    for b in range(C):
        final(jnp.where(leans_left, C - 1 - b, b))

    with jax.named_scope("drain"):
        for x in range(C):
            pl.when((p == x) & has_right)(lambda: all_of(every.at[pl.ds(0, (x + 1) * R), :], ag_send.at[0]))
            pl.when((p == x) & has_left)(lambda: all_of(every.at[pl.ds(0, (C - x) * R), :], ag_send.at[1]))
        all_of(every.at[pl.ds(0, C * R), :], ag_send.at[2])
        all_of(dwv.at[1], down_send)
        all_of(mine.at[:, pl.ds(0, C - 1)], rs_send)


def on_device(n, tokens, norm_gain, gate_weight, up_weight, down_weight):
    S = SUBS
    R, D = tokens.shape
    F = gate_weight.shape[1]
    C = n // 2
    T, W = 2 * R, D // n
    any_space, vmem = pl.BlockSpec(memory_space=pl.ANY), pl.BlockSpec(memory_space=pltpu.VMEM)
    dma = pltpu.SemaphoreType.DMA
    mixed = pl.pallas_call(
        functools.partial(block_kernel, n),
        out_shape=pltpu.VMEM((n * R, W), bf16),
        in_specs=[any_space] * 5,
        out_specs=vmem,
        scratch_shapes=[
            pltpu.VMEM((2, D, F), bf16),
            pltpu.VMEM((2, F, D // 2), bf16),
            pltpu.VMEM((1, D), f32),
            pltpu.VMEM((C * T, D), bf16),
            pltpu.VMEM((T, D), bf16),
            pltpu.VMEM((S, T, 128), f32),
            pltpu.VMEM((2, T, F), f32),
            pltpu.VMEM((2, T, F), bf16),
            pltpu.VMEM((2, T, F), bf16),
            pltpu.VMEM((C, T, W), f32),
            pltpu.VMEM((C, C, T, W), bf16),
            pltpu.VMEM((C, C + 1, T, W), bf16),
            pltpu.VMEM((T, W), bf16),
            pltpu.VMEM((C * T, W), f32),
            dma((S + 1,)),
            dma((2,)),
            dma((C, S, 2)),
            dma((3,)),
            dma,
            dma((2, 2)),
            dma,
            dma,
            dma,
            dma((C, C + 1)),
            dma,
        ],
        compiler_params=pltpu.CompilerParams(collective_id=0, has_side_effects=True, vmem_limit_bytes=VMEM_LIMIT),
    )(tokens, norm_gain[None, :], gate_weight, up_weight, down_weight)
    return mixed


def solution(mesh):
    return jax.shard_map(
        functools.partial(on_device, mesh.shape["tensor"]),
        mesh=mesh,
        in_specs=(
            P(("dp", "tensor"), None),
            P(),
            P(None, "tensor"),
            P(None, "tensor"),
            P("tensor", None),
        ),
        out_specs=P("dp", "tensor"),
        check_vma=False,
    )
```

```python
import functools

import jax
import jax.numpy as jnp
from jax import lax
from jax.experimental import pallas as pl
from jax.experimental.pallas import tpu as pltpu
from jax.sharding import PartitionSpec as P

SUBS = 2
VMEM_LIMIT = 63963136
f32, bf16 = jnp.float32, jnp.bfloat16


def tile_of(F):
    return next(t for t in (256, 128) if F % t == 0)


def block_kernel(
    n, tok, gain, gw, uw, dw, out,
    wide, dwv, gainv, every, normed, sums, partial, hidden, other, half, mine, arrived, far, acc,
    load_sem, own_sem, ag_recv, ag_send, pair_send, pair_recv, down_send, down_recv, rs_send, rs_recv, far_recv,
):
    S = SUBS
    dp = lax.axis_index("dp")
    me = lax.axis_index("tensor")
    C = n // 2
    p, c = me // 2, me % 2
    R, D = tok.shape
    Dc = D // S
    T = 2 * R
    F = wide.shape[2]
    W = D // n
    tile = tile_of(F)
    tiles = F // tile
    cuts = [0, tiles - tiles // 3, tiles]
    partner = (dp, 2 * p + (1 - c))
    right = (dp, lax.rem(me + 2, n))
    left = (dp, lax.rem(me + n - 2, n))
    has_right, has_left = p < C - 1, p > 0
    inner = has_right & has_left
    outer = jnp.logical_not(inner)
    late = C == 4
    leans_left = 2 * p < C - 1
    near = jnp.where(leans_left, -1, 1)
    both = jnp.where(leans_left, p, C - 1 - p)

    def rows_of(b, q):
        return pl.ds(pl.multiple_of((b * 2 + q) * R, R), R)

    def features(j):
        return pl.ds(j * Dc, Dc)

    def block_rows(b):
        return pl.ds(pl.multiple_of(b * T, T), T)

    def columns(t):
        return pl.ds(pl.multiple_of(t * W, W), W)

    own = [pltpu.make_async_copy(tok.at[:, features(j)], every.at[rows_of(p, c), features(j)], own_sem.at[0]) for j in range(S)]
    gain_copy = pltpu.make_async_copy(gain, gainv, own_sem.at[1])

    def load_wide(j):
        return [pltpu.make_async_copy((gw, uw)[x].at[features(j), :], wide.at[x, features(j), :], load_sem.at[j]) for x in range(2)]

    def load_down(d):
        return pltpu.make_async_copy(dw.at[:, columns(2 * d + c)], dwv.at[0, :, pl.ds(d * W, W)], load_sem.at[S])

    def all_of(ref, sem):
        pltpu.make_async_copy(ref, ref, sem).wait()

    def wide_loaded(i):
        all_of(wide.at[:, features(i), :], load_sem.at[i])

    for copy in own:
        copy.start()
    gain_copy.start()

    barrier = pltpu.get_barrier_semaphore()

    def greet(device):
        pl.semaphore_signal(barrier, inc=1, device_id=device, device_id_type=pl.DeviceIdType.MESH)

    greet(partner)
    pl.when(has_right)(lambda: greet(right))
    pl.when(has_left)(lambda: greet(left))
    with jax.named_scope("own"):
        all_of(every.at[pl.ds(0, R), :], own_sem.at[0])
    for i in range(S):
        for copy in load_wide(i):
            copy.start()
    with jax.named_scope("barrier"):
        pl.semaphore_wait(barrier, 1 + has_right.astype(jnp.int32) + has_left.astype(jnp.int32))

    def remote(src, dst, s, d, device):
        return pltpu.make_async_remote_copy(
            src_ref=src, dst_ref=dst, send_sem=s, recv_sem=d, device_id=device, device_id_type=pl.DeviceIdType.MESH
        )

    def gather(b, j, way):
        at = every.at[rows_of(b, c), features(j)]
        return remote(at, at, ag_send.at[way], ag_recv.at[b, j, c], (right, left, partner)[way])

    def gathered(b, j, q):
        at = every.at[rows_of(b, q), features(j)]
        remote(at, at, ag_send.at[2], ag_recv.at[b, j, q], partner).wait_recv()

    @jax.named_scope("relay")
    def relay(k, j):
        @pl.when(p - k >= 0)
        def _():
            gathered(p - k, j, c)
            pl.when(has_right)(lambda: gather(p - k, j, 0).start())
            gather(p - k, j, 2).start()

        @pl.when(p + k <= C - 1)
        def _():
            gathered(p + k, j, c)
            pl.when(has_left)(lambda: gather(p + k, j, 1).start())
            gather(p + k, j, 2).start()

    def share_down(d):
        return remote(dw.at[:, columns(2 * d + 1 - c)], dwv.at[1, :, pl.ds(d * W, W)], down_send, down_recv, partner)

    def share_hidden(s, i):
        at = pl.ds(cuts[i] * tile, (cuts[i + 1] - cuts[i]) * tile)
        return remote(hidden.at[s % 2, :, at], other.at[s % 2, :, at], pair_send, pair_recv.at[s % 2, i], partner)

    def to_right(b, d):
        return remote(mine.at[b, d], arrived.at[b, d + 1], rs_send, rs_recv.at[b, d + 1], right)

    def to_left(b, d):
        return remote(mine.at[b, d], arrived.at[b, d], rs_send, rs_recv.at[b, d], left)

    def to_far(b, d):
        return remote(mine.at[b, d], far, rs_send, far_recv, (dp, 2 * d + c))

    def landed(b, slot):
        remote(arrived.at[b, slot], arrived.at[b, slot], rs_send, rs_recv.at[b, slot], partner).wait_recv()

    def landed_far():
        remote(far, far, rs_send, far_recv, partner).wait_recv()

    def straight_right(b, d):
        return (C > 2) & (b == C - 1) & (d == C - 1)

    def straight_left(b, d):
        return (C > 2) & (b == 0) & (d == 0)

    def first_send(b, d):
        straight = straight_right(b, d)
        pl.when((p == 0) & straight)(lambda: to_far(b, d).start())
        pl.when((d > p) & jnp.where(straight, p == 1, p == 0))(lambda: to_right(b, d).start())
        straight = straight_left(b, d)
        pl.when((p == C - 1) & straight)(lambda: to_far(b, d).start())
        pl.when((d < p) & jnp.where(straight, p == C - 2, p == C - 1))(lambda: to_left(b, d).start())

    def add_to_mine(b, d, slot):
        landed(b, slot)
        mine[b, d] = (mine[b, d].astype(f32) + arrived[b, slot].astype(f32)).astype(bf16)

    @jax.named_scope("right")
    def forward_right(b, targets=range(C - 1, 0, -1)):
        for d in targets:
            @pl.when((d > p) & jnp.logical_not((p == 1) & straight_right(b, d)))
            def _():
                add_to_mine(b, d, d + 1)
                to_right(b, d).start()

    @jax.named_scope("left")
    def forward_left(b, targets=range(C - 1)):
        for d in targets:
            @pl.when((d < p) & jnp.logical_not((p == C - 2) & straight_left(b, d)))
            def _():
                add_to_mine(b, d, d)
                to_left(b, d).start()

    def early_right(b, part):
        ahead = slice(0, 1) if part == 0 else slice(1, None)
        pl.when((p == 1) & has_right)(lambda: forward_right(b, range(C - 1, 0, -1)[ahead]))

    def early_left(b, part):
        ahead = slice(0, 1) if part == 0 else slice(1, None)
        pl.when((p == C - 2) & has_left)(lambda: forward_left(C - 1 - b, range(C - 1)[ahead]))

    def early(b, part):
        early_right(b, part)
        early_left(b, part)

    def earlier():
        pl.when((p == 2) & has_right)(lambda: forward_right(1))
        pl.when((p == C - 3) & has_left)(lambda: forward_left(C - 2))

    def add_to_out(b, ref):
        acc[block_rows(b), :] += ref[...].astype(f32)

    @jax.named_scope("final")
    def final(b):
        @pl.when(has_left)
        def _():
            landed(b, p + 1)
            add_to_out(b, arrived.at[b, p + 1])

        @pl.when(has_right)
        def _():
            landed(b, p)
            add_to_out(b, arrived.at[b, p])

        @pl.when(straight_right(b, p) | straight_left(b, p))
        def _():
            landed_far()
            add_to_out(b, far)

        out[block_rows(b), :] = acc[block_rows(b), :].astype(bf16)

    @jax.named_scope("norm")
    def prepare(b, j, q):
        rows = every[rows_of(b, q), features(j)].astype(f32)
        at = rows_of(0, q)
        sums[j, at, :] = jnp.broadcast_to(jnp.sum(rows * rows, axis=1, keepdims=True), (R, 128))
        normed[at, features(j)] = (rows * gainv[:, features(j)]).astype(bf16)

    def expand(b, s, k):
        def other_rows(j):
            with jax.named_scope("await"):
                gathered(b, j, 1 - c)

        def products(x, j):
            at = pl.ds(x * tile, tile)
            return [jnp.dot(normed[:, features(j)], wide[y, features(j), at], preferred_element_type=f32) for y in range(2)]

        pl.when(s == 0)(lambda: gain_copy.wait())
        for j in range(S - 1):
            prepare(b, j, c)
            other_rows(j)
            prepare(b, j, 1 - c)
            if j == S - 2:
                pl.when(inner & (s >= 1) & (k == s))(lambda: relay(s, S - 1))

            @pl.when(s == 0)
            def _():
                with jax.named_scope("load"):
                    wide_loaded(j)
                    if j == 0:
                        for d in range(C):
                            load_down(d).start()

            with jax.named_scope("expand0"):
                for x in range(tiles):
                    at = pl.ds(x * tile, tile)
                    for y, product in enumerate(products(x, j)):
                        partial[y, :, at] = product if j == 0 else partial[y, :, at] + product
        pl.when(outer & (s >= 1))(lambda: relay(s, S - 1))
        prepare(b, S - 1, c)
        other_rows(S - 1)
        prepare(b, S - 1, 1 - c)

        @pl.when(s == 0)
        def _():
            with jax.named_scope("load"):
                wide_loaded(S - 1)

        def part(i):
            scale = 1.0 / jnp.sqrt(sum(sums[j] for j in range(S)) / D + 1e-05)
            scale = jnp.concatenate([scale] * (tile // 128), axis=1)
            for x in range(cuts[i], cuts[i + 1]):
                at = pl.ds(x * tile, tile)
                gate, up = [(partial[y, :, at] + product) * scale for y, product in enumerate(products(x, S - 1))]
                hidden[s % 2, :, at] = (jax.nn.silu(gate) * up).astype(bf16)

        with jax.named_scope("expand1"):
            part(0)
        share_hidden(s, 0).start()
        pl.when(inner & (s >= 2) & (k != s))(lambda: relay(s, S - 1))
        with jax.named_scope("expand2"):
            part(1)
        share_hidden(s, 1).start()

    def down(b, s):
        turned = (p == 1) & (b == C - 1) if late else p < 0
        far_block = jnp.where(leans_left, (p == 0) & (b == C - 1), (p == C - 1) & (b == 0)) & (C > 2)

        def dest(i):
            i = jnp.where(far_block, 1 - i, i) if i < 2 else i
            return jnp.where(leans_left & jnp.logical_not(turned), C - 1 - i, i)

        def product(of, x, d):
            weight = dwv[x, :, pl.ds(pl.multiple_of(d * W, W), W)]
            return jnp.dot(of[s % 2], weight, preferred_element_type=f32)

        @pl.when(s == 0)
        def _():
            with jax.named_scope("load"):
                all_of(dwv.at[0], load_sem.at[S])

        with jax.named_scope("down0"):
            for d in range(C):
                half[d] = product(hidden, 0, d)

        @pl.when(s == 0)
        def _():
            with jax.named_scope("load"):
                remote(dwv.at[1], dwv.at[1], down_send, down_recv, partner).wait_recv()

        pl.when((s >= 1) & (s + 1 <= C - 1))(lambda: relay(s + 1, 0))
        pl.when(s >= 2)(lambda: early_right(s - 1, 0))
        with jax.named_scope("peer"):
            for i in range(2):
                share_hidden(s, i).wait_recv()
        for at in (range(1), range(1, C)):
            with jax.named_scope("down1"):
                for i in at:
                    d = dest(i)
                    mine[b, d] = (half[d] + product(other, 1, d)).astype(bf16)
            for i in at:
                first_send(b, dest(i))
            if late and len(at) == 1:
                pl.when(turned)(lambda: forward_left(C - 1))
        all_of(hidden.at[s % 2], pair_send)

        acc[block_rows(b), :] = every[block_rows(b), columns(me)].astype(f32) + mine[b, p].astype(f32)

    for j in range(S):
        pl.when(has_right)(lambda: gather(p, j, 0).start())
        pl.when(has_left)(lambda: gather(p, j, 1).start())
        gather(p, j, 2).start()
    for d in range(C):
        share_down(d).start()

    @pl.loop(0, C)
    def _(s):
        k = jnp.where(s <= 2 * both, (s + 1) // 2, s - both)
        side = jnp.where((s <= 2 * both) & (s % 2 == 1), near, -near)
        b = p + side * k

        def other_rows(j):
            with jax.named_scope("await"):
                gathered(b, j, 1 - c)

        expand(b, s, k)
        pl.when(s == 0)(lambda: relay(1, 0))
        pl.when(s >= 2)(lambda: early_left(s - 1, 0))
        pl.when(s == 3)(lambda: earlier())
        down(b, s)
        pl.when(s == 1)(lambda: early(0, 0))
        pl.when((s >= 1) & (s <= C - 2))(lambda: early(s - 1, 1))

    for b in range(C):
        done = ((p == 1) & ((b <= C - 2) | late)) | ((p == 2) & (b == 1) & (C > 3))
        pl.when(inner & jnp.logical_not(done))(lambda: forward_right(b))
        done = ((p == C - 2) & ((b <= C - 2) | late)) | ((p == C - 3) & ((b == 1) & (C > 3) | (b == 0) & late))
        pl.when(inner & jnp.logical_not(done))(lambda: forward_left(C - 1 - b))
        if b == 0:
            early(C - 2, 1)
    if late:
        pl.when(p == 1)(lambda: forward_right(C - 1))
        pl.when(p == C - 2)(lambda: forward_left(0))
    for b in range(C):
        final(jnp.where(leans_left, C - 1 - b, b))

    with jax.named_scope("drain"):
        for x in range(C):
            pl.when((p == x) & has_right)(lambda: all_of(every.at[pl.ds(0, (x + 1) * R), :], ag_send.at[0]))
            pl.when((p == x) & has_left)(lambda: all_of(every.at[pl.ds(0, (C - x) * R), :], ag_send.at[1]))
        all_of(every.at[pl.ds(0, C * R), :], ag_send.at[2])
        all_of(dwv.at[1], down_send)
        all_of(mine.at[:, pl.ds(0, C - 1)], rs_send)


def on_device(n, tokens, norm_gain, gate_weight, up_weight, down_weight):
    S = SUBS
    R, D = tokens.shape
    F = gate_weight.shape[1]
    C = n // 2
    T, W = 2 * R, D // n
    any_space, vmem = pl.BlockSpec(memory_space=pl.ANY), pl.BlockSpec(memory_space=pltpu.VMEM)
    dma = pltpu.SemaphoreType.DMA
    mixed = pl.pallas_call(
        functools.partial(block_kernel, n),
        out_shape=pltpu.VMEM((n * R, W), bf16),
        in_specs=[any_space] * 5,
        out_specs=vmem,
        scratch_shapes=[
            pltpu.VMEM((2, D, F), bf16),
            pltpu.VMEM((2, F, D // 2), bf16),
            pltpu.VMEM((1, D), f32),
            pltpu.VMEM((C * T, D), bf16),
            pltpu.VMEM((T, D), bf16),
            pltpu.VMEM((S, T, 128), f32),
            pltpu.VMEM((2, T, F), f32),
            pltpu.VMEM((2, T, F), bf16),
            pltpu.VMEM((2, T, F), bf16),
            pltpu.VMEM((C, T, W), f32),
            pltpu.VMEM((C, C, T, W), bf16),
            pltpu.VMEM((C, C + 1, T, W), bf16),
            pltpu.VMEM((T, W), bf16),
            pltpu.VMEM((C * T, W), f32),
            dma((S + 1,)),
            dma((2,)),
            dma((C, S, 2)),
            dma((3,)),
            dma,
            dma((2, 2)),
            dma,
            dma,
            dma,
            dma((C, C + 1)),
            dma,
        ],
        compiler_params=pltpu.CompilerParams(collective_id=0, has_side_effects=True, vmem_limit_bytes=VMEM_LIMIT),
    )(tokens, norm_gain[None, :], gate_weight, up_weight, down_weight)
    return mixed


def solution(mesh):
    return jax.shard_map(
        functools.partial(on_device, mesh.shape["tensor"]),
        mesh=mesh,
        in_specs=(
            P(("dp", "tensor"), None),
            P(),
            P(None, "tensor"),
            P(None, "tensor"),
            P("tensor", None),
        ),
        out_specs=P("dp", "tensor"),
        check_vma=False,
    )
```

```python
import functools

import jax
import jax.numpy as jnp
from jax import lax
from jax.experimental import pallas as pl
from jax.experimental.pallas import tpu as pltpu
from jax.sharding import PartitionSpec as P

SUBS = 2
VMEM_LIMIT = 63963136
f32, bf16 = jnp.float32, jnp.bfloat16


def tile_of(F):
    return next(t for t in (256, 128) if F % t == 0)


def block_kernel(
    n, tok, gain, gw, uw, dw, out,
    wide, dwv, gainv, every, normed, sums, partial, hidden, other, half, mine, arrived, far, acc,
    load_sem, own_sem, ag_recv, ag_send, pair_send, pair_recv, down_send, down_recv, rs_send, rs_recv, far_recv,
):
    S = SUBS
    dp = lax.axis_index("dp")
    me = lax.axis_index("tensor")
    C = n // 2
    p, c = me // 2, me % 2
    R, D = tok.shape
    Dc = D // S
    T = 2 * R
    F = wide.shape[2]
    W = D // n
    tile = tile_of(F)
    tiles = F // tile
    cuts = [0, tiles - tiles // 3, tiles]
    partner = (dp, 2 * p + (1 - c))
    right = (dp, lax.rem(me + 2, n))
    left = (dp, lax.rem(me + n - 2, n))
    has_right, has_left = p < C - 1, p > 0
    inner = has_right & has_left
    outer = jnp.logical_not(inner)
    late = C == 4
    leans_left = 2 * p < C - 1
    near = jnp.where(leans_left, -1, 1)
    both = jnp.where(leans_left, p, C - 1 - p)

    def rows_of(b, q):
        return pl.ds(pl.multiple_of((b * 2 + q) * R, R), R)

    def features(j):
        return pl.ds(j * Dc, Dc)

    def block_rows(b):
        return pl.ds(pl.multiple_of(b * T, T), T)

    def columns(t):
        return pl.ds(pl.multiple_of(t * W, W), W)

    own = [pltpu.make_async_copy(tok.at[:, features(j)], every.at[rows_of(p, c), features(j)], own_sem.at[0]) for j in range(S)]
    gain_copy = pltpu.make_async_copy(gain, gainv, own_sem.at[1])

    def load_wide(j):
        return [pltpu.make_async_copy((gw, uw)[x].at[features(j), :], wide.at[x, features(j), :], load_sem.at[j]) for x in range(2)]

    def load_down(d):
        return pltpu.make_async_copy(dw.at[:, columns(2 * d + c)], dwv.at[0, :, pl.ds(d * W, W)], load_sem.at[S])

    def all_of(ref, sem):
        pltpu.make_async_copy(ref, ref, sem).wait()

    def wide_loaded(i):
        all_of(wide.at[:, features(i), :], load_sem.at[i])

    for copy in own:
        copy.start()
    gain_copy.start()

    barrier = pltpu.get_barrier_semaphore()

    def greet(device):
        pl.semaphore_signal(barrier, inc=1, device_id=device, device_id_type=pl.DeviceIdType.MESH)

    greet(partner)
    pl.when(has_right)(lambda: greet(right))
    pl.when(has_left)(lambda: greet(left))
    with jax.named_scope("own"):
        all_of(every.at[pl.ds(0, R), :], own_sem.at[0])
    for i in range(S):
        for copy in load_wide(i):
            copy.start()
    with jax.named_scope("barrier"):
        pl.semaphore_wait(barrier, 1 + has_right.astype(jnp.int32) + has_left.astype(jnp.int32))

    def remote(src, dst, s, d, device):
        return pltpu.make_async_remote_copy(
            src_ref=src, dst_ref=dst, send_sem=s, recv_sem=d, device_id=device, device_id_type=pl.DeviceIdType.MESH
        )

    def gather(b, j, way):
        at = every.at[rows_of(b, c), features(j)]
        return remote(at, at, ag_send.at[way], ag_recv.at[b, j, c], (right, left, partner)[way])

    def gathered(b, j, q):
        at = every.at[rows_of(b, q), features(j)]
        remote(at, at, ag_send.at[2], ag_recv.at[b, j, q], partner).wait_recv()

    @jax.named_scope("relay")
    def relay(k, j):
        @pl.when(p - k >= 0)
        def _():
            gathered(p - k, j, c)
            pl.when(has_right)(lambda: gather(p - k, j, 0).start())
            gather(p - k, j, 2).start()

        @pl.when(p + k <= C - 1)
        def _():
            gathered(p + k, j, c)
            pl.when(has_left)(lambda: gather(p + k, j, 1).start())
            gather(p + k, j, 2).start()

    def share_down(d):
        return remote(dw.at[:, columns(2 * d + 1 - c)], dwv.at[1, :, pl.ds(d * W, W)], down_send, down_recv, partner)

    def share_hidden(s, i):
        at = pl.ds(cuts[i] * tile, (cuts[i + 1] - cuts[i]) * tile)
        return remote(hidden.at[s % 2, :, at], other.at[s % 2, :, at], pair_send, pair_recv.at[s % 2, i], partner)

    def to_right(b, d):
        return remote(mine.at[b, d], arrived.at[b, d + 1], rs_send, rs_recv.at[b, d + 1], right)

    def to_left(b, d):
        return remote(mine.at[b, d], arrived.at[b, d], rs_send, rs_recv.at[b, d], left)

    def to_far(b, d):
        return remote(mine.at[b, d], far, rs_send, far_recv, (dp, 2 * d + c))

    def landed(b, slot):
        remote(arrived.at[b, slot], arrived.at[b, slot], rs_send, rs_recv.at[b, slot], partner).wait_recv()

    def landed_far():
        remote(far, far, rs_send, far_recv, partner).wait_recv()

    def straight_right(b, d):
        return (C > 2) & (b == C - 1) & (d == C - 1)

    def straight_left(b, d):
        return (C > 2) & (b == 0) & (d == 0)

    def first_send(b, d):
        straight = straight_right(b, d)
        pl.when((p == 0) & straight)(lambda: to_far(b, d).start())
        pl.when((d > p) & jnp.where(straight, p == 1, p == 0))(lambda: to_right(b, d).start())
        straight = straight_left(b, d)
        pl.when((p == C - 1) & straight)(lambda: to_far(b, d).start())
        pl.when((d < p) & jnp.where(straight, p == C - 2, p == C - 1))(lambda: to_left(b, d).start())

    def add_to_mine(b, d, slot):
        landed(b, slot)
        mine[b, d] = (mine[b, d].astype(f32) + arrived[b, slot].astype(f32)).astype(bf16)

    @jax.named_scope("right")
    def forward_right(b, targets=range(C - 1, 0, -1)):
        for d in targets:
            @pl.when((d > p) & jnp.logical_not((p == 1) & straight_right(b, d)))
            def _():
                add_to_mine(b, d, d + 1)
                to_right(b, d).start()

    @jax.named_scope("left")
    def forward_left(b, targets=range(C - 1)):
        for d in targets:
            @pl.when((d < p) & jnp.logical_not((p == C - 2) & straight_left(b, d)))
            def _():
                add_to_mine(b, d, d)
                to_left(b, d).start()

    def early_right(b, part):
        ahead = slice(0, 1) if part == 0 else slice(1, None)
        pl.when((p == 1) & has_right)(lambda: forward_right(b, range(C - 1, 0, -1)[ahead]))

    def early_left(b, part):
        ahead = slice(0, 1) if part == 0 else slice(1, None)
        pl.when((p == C - 2) & has_left)(lambda: forward_left(C - 1 - b, range(C - 1)[ahead]))

    def early(b, part):
        early_right(b, part)
        early_left(b, part)

    def earlier():
        pl.when((p == 2) & has_right)(lambda: forward_right(1))
        pl.when((p == C - 3) & has_left)(lambda: forward_left(C - 2))

    def add_to_out(b, ref):
        acc[block_rows(b), :] += ref[...].astype(f32)

    @jax.named_scope("final")
    def final(b):
        @pl.when(has_left)
        def _():
            landed(b, p + 1)
            add_to_out(b, arrived.at[b, p + 1])

        @pl.when(has_right)
        def _():
            landed(b, p)
            add_to_out(b, arrived.at[b, p])

        @pl.when(straight_right(b, p) | straight_left(b, p))
        def _():
            landed_far()
            add_to_out(b, far)

        out[block_rows(b), :] = acc[block_rows(b), :].astype(bf16)

    @jax.named_scope("norm")
    def prepare(b, j, q):
        rows = every[rows_of(b, q), features(j)].astype(f32)
        at = rows_of(0, q)
        sums[j, at, :] = jnp.broadcast_to(jnp.sum(rows * rows, axis=1, keepdims=True), (R, 128))
        normed[at, features(j)] = (rows * gainv[:, features(j)]).astype(bf16)

    def expand(b, s, k):
        def other_rows(j):
            with jax.named_scope("await"):
                gathered(b, j, 1 - c)

        def products(x, j):
            at = pl.ds(x * tile, tile)
            return [jnp.dot(normed[:, features(j)], wide[y, features(j), at], preferred_element_type=f32) for y in range(2)]

        pl.when(s == 0)(lambda: gain_copy.wait())
        for j in range(S - 1):
            prepare(b, j, c)
            other_rows(j)
            prepare(b, j, 1 - c)
            if j == S - 2:
                pl.when(s == 1)(lambda: relay(s, S - 1))

            @pl.when(s == 0)
            def _():
                with jax.named_scope("load"):
                    wide_loaded(j)
                    if j == 0:
                        for d in range(C):
                            load_down(d).start()

            with jax.named_scope("expand0"):
                for x in range(tiles):
                    at = pl.ds(x * tile, tile)
                    for y, product in enumerate(products(x, j)):
                        partial[y, :, at] = product if j == 0 else partial[y, :, at] + product
        pl.when(outer & (s >= 2))(lambda: relay(s, S - 1))
        prepare(b, S - 1, c)
        other_rows(S - 1)
        prepare(b, S - 1, 1 - c)

        @pl.when(s == 0)
        def _():
            with jax.named_scope("load"):
                wide_loaded(S - 1)

        def part(i):
            scale = 1.0 / jnp.sqrt(sum(sums[j] for j in range(S)) / D + 1e-05)
            scale = jnp.concatenate([scale] * (tile // 128), axis=1)
            for x in range(cuts[i], cuts[i + 1]):
                at = pl.ds(x * tile, tile)
                gate, up = [(partial[y, :, at] + product) * scale for y, product in enumerate(products(x, S - 1))]
                hidden[s % 2, :, at] = (jax.nn.silu(gate) * up).astype(bf16)

        with jax.named_scope("expand1"):
            part(0)
        share_hidden(s, 0).start()
        pl.when(inner & (s >= 2) & (k != s))(lambda: relay(s, S - 1))
        with jax.named_scope("expand2"):
            part(1)
        share_hidden(s, 1).start()

    def down(b, s):
        turned = (p == 1) & (b == C - 1) if late else p < 0
        far_block = jnp.where(leans_left, (p == 0) & (b == C - 1), (p == C - 1) & (b == 0)) & (C > 2)

        def dest(i):
            i = jnp.where(far_block, 1 - i, i) if i < 2 else i
            return jnp.where(leans_left & jnp.logical_not(turned), C - 1 - i, i)

        def product(of, x, d):
            weight = dwv[x, :, pl.ds(pl.multiple_of(d * W, W), W)]
            return jnp.dot(of[s % 2], weight, preferred_element_type=f32)

        @pl.when(s == 0)
        def _():
            with jax.named_scope("load"):
                all_of(dwv.at[0], load_sem.at[S])

        with jax.named_scope("down0"):
            for d in range(C):
                half[d] = product(hidden, 0, d)

        @pl.when(s == 0)
        def _():
            with jax.named_scope("load"):
                remote(dwv.at[1], dwv.at[1], down_send, down_recv, partner).wait_recv()

        pl.when((s >= 1) & (s + 1 <= C - 1))(lambda: relay(s + 1, 0))
        pl.when(s >= 2)(lambda: early_right(s - 1, 0))
        with jax.named_scope("peer"):
            for i in range(2):
                share_hidden(s, i).wait_recv()
        for at in (range(1), range(1, C)):
            with jax.named_scope("down1"):
                for i in at:
                    d = dest(i)
                    mine[b, d] = (half[d] + product(other, 1, d)).astype(bf16)
            for i in at:
                first_send(b, dest(i))
            if late and len(at) == 1:
                pl.when(turned)(lambda: forward_left(C - 1))
        all_of(hidden.at[s % 2], pair_send)

        acc[block_rows(b), :] = every[block_rows(b), columns(me)].astype(f32) + mine[b, p].astype(f32)

    for j in range(S):
        pl.when(has_right)(lambda: gather(p, j, 0).start())
        pl.when(has_left)(lambda: gather(p, j, 1).start())
        gather(p, j, 2).start()
    for d in range(C):
        share_down(d).start()

    @pl.loop(0, C)
    def _(s):
        k = jnp.where(s <= 2 * both, (s + 1) // 2, s - both)
        side = jnp.where((s <= 2 * both) & (s % 2 == 1), near, -near)
        b = p + side * k

        def other_rows(j):
            with jax.named_scope("await"):
                gathered(b, j, 1 - c)

        expand(b, s, k)
        pl.when(s == 0)(lambda: relay(1, 0))
        pl.when(s >= 2)(lambda: early_left(s - 1, 0))
        pl.when(s == 3)(lambda: earlier())
        down(b, s)
        pl.when(s == 1)(lambda: early(0, 0))
        pl.when((s >= 1) & (s <= C - 2))(lambda: early(s - 1, 1))

    for b in range(C):
        done = ((p == 1) & ((b <= C - 2) | late)) | ((p == 2) & (b == 1) & (C > 3))
        pl.when(inner & jnp.logical_not(done))(lambda: forward_right(b))
        done = ((p == C - 2) & ((b <= C - 2) | late)) | ((p == C - 3) & ((b == 1) & (C > 3) | (b == 0) & late))
        pl.when(inner & jnp.logical_not(done))(lambda: forward_left(C - 1 - b))
        if b == 0:
            early(C - 2, 1)
    if late:
        pl.when(p == 1)(lambda: forward_right(C - 1))
        pl.when(p == C - 2)(lambda: forward_left(0))
    for b in range(C):
        final(jnp.where(leans_left, C - 1 - b, b))

    with jax.named_scope("drain"):
        for x in range(C):
            pl.when((p == x) & has_right)(lambda: all_of(every.at[pl.ds(0, (x + 1) * R), :], ag_send.at[0]))
            pl.when((p == x) & has_left)(lambda: all_of(every.at[pl.ds(0, (C - x) * R), :], ag_send.at[1]))
        all_of(every.at[pl.ds(0, C * R), :], ag_send.at[2])
        all_of(dwv.at[1], down_send)
        all_of(mine.at[:, pl.ds(0, C - 1)], rs_send)


def on_device(n, tokens, norm_gain, gate_weight, up_weight, down_weight):
    S = SUBS
    R, D = tokens.shape
    F = gate_weight.shape[1]
    C = n // 2
    T, W = 2 * R, D // n
    any_space, vmem = pl.BlockSpec(memory_space=pl.ANY), pl.BlockSpec(memory_space=pltpu.VMEM)
    dma = pltpu.SemaphoreType.DMA
    mixed = pl.pallas_call(
        functools.partial(block_kernel, n),
        out_shape=pltpu.VMEM((n * R, W), bf16),
        in_specs=[any_space] * 5,
        out_specs=vmem,
        scratch_shapes=[
            pltpu.VMEM((2, D, F), bf16),
            pltpu.VMEM((2, F, D // 2), bf16),
            pltpu.VMEM((1, D), f32),
            pltpu.VMEM((C * T, D), bf16),
            pltpu.VMEM((T, D), bf16),
            pltpu.VMEM((S, T, 128), f32),
            pltpu.VMEM((2, T, F), f32),
            pltpu.VMEM((2, T, F), bf16),
            pltpu.VMEM((2, T, F), bf16),
            pltpu.VMEM((C, T, W), f32),
            pltpu.VMEM((C, C, T, W), bf16),
            pltpu.VMEM((C, C + 1, T, W), bf16),
            pltpu.VMEM((T, W), bf16),
            pltpu.VMEM((C * T, W), f32),
            dma((S + 1,)),
            dma((2,)),
            dma((C, S, 2)),
            dma((3,)),
            dma,
            dma((2, 2)),
            dma,
            dma,
            dma,
            dma((C, C + 1)),
            dma,
        ],
        compiler_params=pltpu.CompilerParams(collective_id=0, has_side_effects=True, vmem_limit_bytes=VMEM_LIMIT),
    )(tokens, norm_gain[None, :], gate_weight, up_weight, down_weight)
    return mixed


def solution(mesh):
    return jax.shard_map(
        functools.partial(on_device, mesh.shape["tensor"]),
        mesh=mesh,
        in_specs=(
            P(("dp", "tensor"), None),
            P(),
            P(None, "tensor"),
            P(None, "tensor"),
            P("tensor", None),
        ),
        out_specs=P("dp", "tensor"),
        check_vma=False,
    )
```
